32 devices in a mesh: kpt: 1, ga: 32 (over z, y, x, core).
Axes of the slice: x: 2, y: 2, z: 4, core: 2. Of those that a mesh axis runs over, the one named last changes fastest.
Arguments:
- orbitals: float32 [2, 1024, 131072], P(None, 'kpt', 'ga'), may hold values from -6 to 6
- coeff_cells: int32 [131072], P('ga'), may hold values from -1 to 2097151, as said below
- potential: float32 [128, 128, 128], P('ga'), may hold values from -6 to 6
Outputs:
- applied: float32 [2, 1, 131072], P(None, 'kpt', 'ga')
- subspace: float32 [1024, 2, 1], P('ga', None, 'kpt')
The draws below stay inside these ranges and needn't reach their ends.
Inputs may be any that keep to these rules, and one draw needn't show every extreme that they name: `coeff_cells`: each block of 4096 entries (one device's) lists whole columns of cells (cells with the same first two coordinates) one after another, each column's cells in rising third coordinate, and then -1 in its remaining slots. The cells listed over all blocks are exactly the cells with f(a)^2 + f(b)^2 + f(c)^2 <= 30^2, each once. The numbers of columns of two blocks differ by one at most.
All inputs are finite; a program needn't handle non-finite values.
Results may differ from the reference program's by a relative error of at most 0.0003.
Values sent between devices are 32-bit elements; how exact they have to be, the bound alone decides.
A program may use at most 128 MiB of HBM per device.

```python
import math
import jax
import jax.numpy as jnp
from jax import lax

NGRID = 128
RADIUS = 30
NG = 131072
NB_ALL = 1024
BANDS = 1
NG_DEV = 4096
N_GA = 32


def draw_coeff_cells(key, part):
    extent = NGRID
    device_count = N_GA
    columns_all = extent * extent
    indices = jnp.arange(extent, dtype=jnp.int32)
    frequency = jnp.where(indices < extent // 2, indices, indices - extent)
    square = frequency * frequency
    column_square = (square[:, None] + square[None, :]).reshape(columns_all)
    inside = square[None, :] <= (RADIUS * RADIUS - column_square)[:, None]
    inside_count = inside.astype(jnp.int32)
    lengths = jnp.sum(inside_count, axis=1)
    shuffle = jax.random.permutation(key, columns_all).astype(jnp.int32)
    scores = lengths * columns_all + shuffle
    ordering = jnp.argsort(-scores).astype(jnp.int32)
    rank_of = jnp.zeros((columns_all,), jnp.int32).at[ordering].set(jnp.arange(columns_all, dtype=jnp.int32))
    rounds = rank_of // device_count
    position = rank_of % device_count
    owners = jnp.where(rounds % 2 == 0, position, device_count - 1 - position)
    sorted_lengths = lengths[ordering]
    sorted_owner = owners[ordering]
    owner_ids = jnp.arange(device_count, dtype=jnp.int32)
    owner_hits = (sorted_owner[:, None] == owner_ids[None, :]).astype(jnp.int32)
    weighted = owner_hits * sorted_lengths[:, None]
    running = jnp.cumsum(weighted, axis=0) - weighted
    sorted_start = jnp.sum(running * owner_hits, axis=1)
    column_start = jnp.zeros((columns_all,), jnp.int32).at[ordering].set(sorted_start)
    within = jnp.cumsum(inside_count, axis=1) - inside_count
    slot_of = owners[:, None] * NG_DEV + column_start[:, None] + within
    slot_of = jnp.where(inside, slot_of, NG)
    cell_ids = jnp.arange(extent ** 3, dtype=jnp.int32).reshape(columns_all, extent)
    filled = jnp.full((NG + 1,), -1, jnp.int32).at[slot_of.reshape(-1)].set(cell_ids.reshape(-1))
    return filled[:NG]


def raised(values, rng, source, target, shards_of, factor):
    def block_of(dim):
        return (jnp.arange(values.shape[dim]) // (values.shape[dim] // shards_of)).reshape((-1,) + (1,) * (values.ndim - 1 - dim))

    near = jax.random.permutation(rng, shards_of)[block_of(target)]
    other_side = (block_of(target) + shards_of // 2) % shards_of
    return jnp.where((block_of(source) == near) | (block_of(source) == other_side), factor * values, values)


def steps_of(stream_key, dims, shards, least, top_value):
    def one(dim, blocks):
        steps = jax.random.uniform(jax.random.fold_in(jax.random.fold_in(stream_key, 6), dim), (blocks,), jnp.float32, least / len(shards), top_value / len(shards))
        return jnp.repeat(jnp.exp(steps), dims[dim] // blocks).reshape((-1,) + (1,) * (len(dims) - dim - 1))

    level = one(*shards[0])
    for cut in shards[1:]:
        level = level * one(*cut)
    return level


def normal_values(rng, shape, scale, reach, split=(), kind=jnp.bfloat16):
    factor_of = steps_of(rng, shape, split, -0.22, 0.18) if split else 1.0
    array = jax.random.normal(rng, shape, jnp.float32) * scale * factor_of
    return jnp.minimum(jnp.maximum(array, -reach), reach).astype(kind)


def heavy_noise(own_key, shape, scale, most, shards, heavy, kind=jnp.bfloat16):
    result = scale * jax.random.normal(own_key, shape, jnp.float32)
    if shards:
        result = result * steps_of(own_key, shape, shards, -0.22, 0.18)
    return jnp.clip(raised(result, jax.random.fold_in(own_key, 3), *heavy), -most, most).astype(kind)


def setup_inputs(seed: int = 0, part: int = 0) -> dict:
    key_of = jax.random.split(jax.random.key(seed), 4)
    own_keys = jax.random.split(jax.random.fold_in(key_of[3], part), 4)
    orbitals = heavy_noise(own_keys[0], (2, NB_ALL, NG), 1.0, 6.0, ((2, 32),), (2, 1, 32, 2.75), jnp.float32)
    coeff_cells = draw_coeff_cells(jax.random.fold_in(key_of[3], 71), part)
    potential = normal_values(key_of[2], (NGRID, NGRID, NGRID), 1.0, 6.0, ((0, 32),), jnp.float32)
    return dict(orbitals=orbitals, coeff_cells=coeff_cells, potential=potential)


def signed_frequency(values):
    return jnp.where(values < NGRID // 2, values, values - NGRID)

def kinetic_of(grid_cells):
    plane_a = grid_cells // (NGRID * NGRID)
    plane_b = grid_cells // NGRID % NGRID
    plane_c = grid_cells % NGRID
    total = signed_frequency(plane_a) ** 2 + signed_frequency(plane_b) ** 2 + signed_frequency(plane_c) ** 2
    return total.astype(jnp.float32) / (RADIUS * RADIUS)

def reference(orbitals, coeff_cells, potential):
    volume = NGRID ** 3
    is_live = coeff_cells >= 0
    live_mask = is_live.astype(jnp.float32)
    target = jnp.where(is_live, coeff_cells, volume).astype(jnp.int32)
    kinetic = kinetic_of(jnp.where(is_live, coeff_cells, 0).astype(jnp.int32)) * live_mask
    real_part = orbitals[0, :BANDS]
    imag_part = orbitals[1, :BANDS]
    norm_root = math.sqrt(NG)

    def one_band(values):
        coeffs = lax.complex(values[0], values[1])
        spread = jnp.zeros((volume + 1,), coeffs.dtype).at[target].set(coeffs)[:volume]
        spread = spread.reshape(NGRID, NGRID, NGRID)
        real_space = jnp.fft.ifftn(spread) * (volume / norm_root)
        products = jnp.fft.fftn(potential * real_space) * (norm_root / volume)
        extended = jnp.concatenate([products.reshape(volume), jnp.zeros((1,), products.dtype)])
        picked = extended[target]
        return (jnp.real(picked), jnp.imag(picked))
    field_real, field_imag = lax.map(one_band, (real_part, imag_part))
    applied_real = kinetic * real_part + field_real
    applied_imag = kinetic * imag_part + field_imag
    applied = jnp.stack([applied_real, applied_imag])
    numbers = (((1,), (1,)), ((), ()))
    highest = lax.Precision.HIGHEST
    tile_real = lax.dot_general(orbitals[0], applied_real, numbers, precision=highest) + lax.dot_general(orbitals[1], applied_imag, numbers, precision=highest)
    tile_imag = lax.dot_general(orbitals[0], applied_imag, numbers, precision=highest) - lax.dot_general(orbitals[1], applied_real, numbers, precision=highest)
    subspace = jnp.stack([tile_real, tile_imag], axis=1) / NG
    return (applied, subspace)
```

```python
import functools

import jax
import jax.numpy as jnp
import ml_dtypes
import numpy as np
from jax import lax
from jax.experimental import pallas as pl
from jax.experimental.pallas import tpu as pltpu
from jax.sharding import PartitionSpec as P

RADIUS = 30
BF = jnp.bfloat16
F32 = jnp.float32
LANES = 128
NN = (((1,), (0,)), ((), ()))
NT = (((1,), (1,)), ((), ()))


def split_np(table):
    high = table.astype(np.float32).astype(ml_dtypes.bfloat16)
    low = (table - high.astype(np.float64)).astype(np.float32).astype(ml_dtypes.bfloat16)
    return high, low


def stack_np(table, axis):
    high, low = split_np(table)
    return np.concatenate([high, high, low], axis=axis)


def phases(extent, half):
    index = np.arange(half)
    freq = np.where(index < half // 2, index, index - half)
    angle = 2.0 * np.pi * ((np.arange(extent)[:, None] * freq[None, :]) % extent) / extent
    return np.cos(angle), np.sin(angle)


@functools.lru_cache(None)
def tables(extent, count, rows_msg):
    half = extent // 2
    layers = extent // count
    cos, sin = phases(extent, half)
    first = np.zeros((count, rows_msg, 2 * half))
    last = np.zeros((2 * half, count, rows_msg))
    for l in range(layers):
        z = np.arange(count) * layers + l
        first[:, l, :half], first[:, l, half:] = cos[z], -sin[z]
        first[:, layers + l, :half], first[:, layers + l, half:] = sin[z], cos[z]
        last[:half, :, l], last[:half, :, layers + l] = cos[z].T, sin[z].T
        last[half:, :, l], last[half:, :, layers + l] = -sin[z].T, cos[z].T
    first = first.reshape(count * rows_msg, 2 * half)
    last = last.reshape(2 * half, count * rows_msg) / float(extent) ** 3
    up_a = np.block([[cos, -sin], [sin, cos]])
    up_b = np.concatenate([cos.T, sin.T], axis=1)
    down_b = np.block([[cos, -sin], [sin, cos]])
    down_a = np.concatenate([cos.T, sin.T], axis=0)
    up_b_high, up_b_low = split_np(up_b)
    return (
        stack_np(first, 1),
        stack_np(up_a, 1),
        np.stack([up_b_high, up_b_low]),
        stack_np(down_b, 0),
        stack_np(down_a, 1),
        stack_np(last, 1),
    )


def dot(left, right, dims=NN):
    return lax.dot_general(left, right, dims, preferred_element_type=F32)


def split(values):
    high = values.astype(BF)
    return high, (values - high.astype(F32)).astype(BF)


def stacked(values, axis):
    high, low = split(values)
    return jnp.concatenate([high, low, high], axis=axis)


def signed(values, extent):
    return jnp.where(values < extent // 2, values, values - extent)


def bits_of(number, width):
    return [lax.rem(lax.div(number, 2**k), 2) for k in range(width)]


def kernel(
    count, layers, extent, rows_msg, group,
    cells_hbm, pot_hbm, first_hbm, up_a_hbm, up_b_hbm, down_b_hbm, down_a_hbm, last_hbm,
    orb_hbm, applied_ref, sub_ref,
    cells_ref, pot_ref, first_ref, up_a_ref, up_b_ref, down_b_ref, down_a_ref, last_ref,
    orb, spread, place, ids_out, ids_in, msg, arrived, pot_out, pot_in,
    slab, pick_b, grid, freq, back, back_in, sums, sub_out, sub_in, kin, colrow, space,
    win_sem, orb_sem, load_sem, send_sem, recv_sem, ids_sem, msg_sem, pot_sem,
):
    me = lax.axis_index("ga")
    half = extent // 2
    slots = orb.shape[2]
    blocks = slots // LANES
    bands_all = orb.shape[1]
    sub_rows = bands_all // count
    parts = 2 * layers
    width = count.bit_length() - 1
    turns = [(1 - 2 * bit) * 2**k for k, bit in enumerate(bits_of(me, width))]

    def peer(step):
        return me + sum([turns[k] for k in range(width) if step >> k & 1], 0)

    def turned(step, low):
        wide = width - low
        return me + sum([bit * turns[low + k] for k, bit in enumerate(bits_of(step, wide))], 0)

    far_first = [peer(step) for step in range(count - 1, 0, -1)]
    barrier = pltpu.get_barrier_semaphore()
    load_cells = pltpu.make_async_copy(cells_hbm, cells_ref, load_sem.at[0])
    load_cells.start()
    head = pltpu.make_async_copy(orb_hbm.at[:, 0:8, :], orb.at[:, 0:8, :], win_sem)
    head.start()
    for other in far_first:
        pl.semaphore_signal(barrier, inc=1, device_id={"ga": other})
    sources = (first_hbm, pot_hbm, up_a_hbm, up_b_hbm, down_b_hbm, down_a_hbm, last_hbm)
    targets = (first_ref, pot_ref, up_a_ref, up_b_ref, down_b_ref, down_a_ref, last_ref)
    loads = [
        pltpu.make_async_copy(source, target, load_sem.at[i + 1])
        for i, (source, target) in enumerate(zip(sources, targets))
    ]
    load_first, load_pot, load_up_a, load_up_b, load_down_b, load_down_a, load_last = loads
    for load in loads:
        load.start()
    rest = pltpu.make_async_copy(orb_hbm.at[:, 8:, :], orb.at[:, 8:, :], orb_sem)
    rest.start()
    groups = count // group
    my_group = me // group

    def exchange(source, target, phase, landed):
        own = pltpu.make_async_copy(source.at[me], target.at[me], landed)
        own.start()

        for other in far_first:
            pltpu.make_async_remote_copy(
                src_ref=source.at[other],
                dst_ref=target.at[me],
                send_sem=send_sem.at[phase],
                recv_sem=landed,
                device_id={"ga": other},
            ).start()

    def arrive(target, phase):
        pltpu.make_async_copy(target, target, recv_sem.at[phase]).wait()

    def sent(source, phase):
        view = source.at[pl.ds(0, count - 1)]
        pltpu.make_async_copy(view, view, send_sem.at[phase]).wait()

    load_cells.wait()
    cells = cells_ref[...]
    live = cells >= 0
    column = jnp.right_shift(cells, extent.bit_length() - 1)
    rolled = pltpu.roll(column, 1, 1)
    lane = lax.broadcasted_iota(jnp.int32, cells.shape, 1)
    row = lax.broadcasted_iota(jnp.int32, cells.shape, 0)
    earlier = jnp.where(lane == 0, pltpu.roll(rolled, 1, 0), rolled)
    earlier = jnp.where((lane == 0) & (row == 0), -1, earlier)
    starts = live & (column != earlier)
    flags = starts.astype(F32).astype(BF)
    sq = lambda axis: lax.broadcasted_iota(jnp.int32, (LANES, LANES), axis)
    upper = (sq(0) <= sq(1)).astype(F32).astype(BF)
    inner = dot(flags, upper)
    totals = dot(flags, jnp.ones((LANES, LANES), BF))
    below = lax.broadcasted_iota(jnp.int32, (blocks, blocks), 1) < lax.broadcasted_iota(
        jnp.int32, (blocks, blocks), 0
    )
    outer = dot(below.astype(F32).astype(BF), totals.astype(BF))
    local = (inner + outer - 1.0).astype(jnp.int32)
    local = jnp.where(live, local, -1)
    safe = jnp.where(live, cells, 0)
    plane_c = safe % extent
    plane_b = safe // extent % extent
    plane_a = safe // (extent * extent)
    fa, fb, fc = signed(plane_a, extent), signed(plane_b, extent), signed(plane_c, extent)
    kinetic = (fa * fa + fb * fb + fc * fc).astype(F32) / (RADIUS * RADIUS)
    kin[...] = jnp.where(live, kinetic, 0.0)
    colrow[0] = local
    colrow[1] = plane_c % half
    colrow[2] = jnp.where(starts, plane_a % half, 0)
    colrow[3] = jnp.where(starts, plane_b % half, 0)

    head.wait()
    sub_half = lax.broadcasted_iota(jnp.int32, (half, LANES), 0)
    sub_full = lax.broadcasted_iota(jnp.int32, (LANES, LANES), 0)
    sub_ids = lax.broadcasted_iota(jnp.int32, (16, LANES), 0)

    def fill(r, carry):
        span = pl.ds(pl.multiple_of(r * LANES, LANES), LANES)
        mine = colrow[0, pl.ds(r, 1), :]
        depth = colrow[1, pl.ds(r, 1), :]
        is_a = colrow[2, pl.ds(r, 1), :].astype(F32)
        is_b = colrow[3, pl.ds(r, 1), :].astype(F32)
        place[0:LANES, span] = jnp.where(sub_full == mine, 1.0, 0.0).astype(BF)
        at_depth = sub_half == depth
        for part in range(2):
            values = orb[part, 0:1, span]
            high, low = split(values)
            spread[2 * part * half : (2 * part + 1) * half, span] = jnp.where(
                at_depth, high.astype(F32), 0.0
            ).astype(BF)
            spread[(2 * part + 1) * half : (2 * part + 2) * half, span] = jnp.where(
                at_depth, low.astype(F32), 0.0
            ).astype(BF)
        tail = jnp.where(sub_ids == 0, is_a, jnp.where(sub_ids == 1, is_b, 0.0))
        spread[4 * half : 4 * half + 16, span] = tail.astype(BF)
        return carry

    lax.fori_loop(0, blocks, fill, 0)
    sticks = dot(spread[...], place[...], NT)
    code = sticks[4 * half : 4 * half + 1] * half + sticks[4 * half + 1 : 4 * half + 2]

    def copy_ids(d, carry):
        ids_out[d] = code
        return carry

    lax.fori_loop(0, count, copy_ids, 0)
    both = jnp.concatenate(
        [
            sticks[0:half] + sticks[half : 2 * half],
            sticks[2 * half : 3 * half] + sticks[3 * half : 4 * half],
        ],
        axis=0,
    )
    load_first.wait()
    msg[...] = dot(first_ref[...], stacked(both, 0)).reshape(count, rows_msg, LANES)
    pl.semaphore_wait(barrier, count - 1)
    exchange(ids_out, ids_in, 0, ids_sem.at[my_group])
    exchange(msg, arrived, 1, msg_sem.at[my_group])

    load_pot.wait()
    for a in range(layers):
        across = jnp.transpose(pot_ref[a])
        for d in range(count):
            for l in range(layers):
                pot_out[l, d, a : a + 1, :] = across[d * layers + l : d * layers + l + 1]
    for l in range(layers):
        exchange(pot_out.at[l], pot_in.at[l], 2, pot_sem.at[l])

    grid[...] = jnp.zeros_like(grid)

    def gather_group(step, carry):
        g = lax.div(turned(step, group.bit_length() - 1), group)
        ids_view = ids_in.at[pl.ds(g * group, group)]
        pltpu.make_async_copy(ids_view, ids_view, ids_sem.at[g]).wait()
        msg_view = arrived.at[pl.ds(g * group, group)]
        pltpu.make_async_copy(msg_view, msg_view, msg_sem.at[g]).wait()
        for k in range(group):
            d = g * group + k
            number = ids_in[d].astype(jnp.int32)
            in_a = sub_half == number // half
            span = pl.ds(k * LANES, LANES)
            pick_b[:, span] = jnp.where(sub_half == number % half, 1.0, 0.0).astype(BF)
            tile = arrived[d]
            high, low = split(tile)
            high, low = high.astype(F32), low.astype(F32)
            for p in range(parts):
                slab[2 * p * half : (2 * p + 1) * half, span] = jnp.where(
                    in_a, high[p : p + 1], 0.0
                ).astype(BF)
                slab[(2 * p + 1) * half : (2 * p + 2) * half, span] = jnp.where(
                    in_a, low[p : p + 1], 0.0
                ).astype(BF)
        grid[...] += dot(slab[...], pick_b[...], NT)
        return carry

    lax.fori_loop(0, groups, gather_group, 0)
    load_up_a.wait()
    load_up_b.wait()
    load_down_b.wait()
    load_down_a.wait()

    for l in range(layers):
        pair = []
        for p in (l, layers + l):
            base = 2 * p * half
            pair.append(grid[base : base + half] + grid[base + half : base + 2 * half])
        lifted = dot(up_a_ref[...], stacked(jnp.concatenate(pair, axis=0), 0))
        high, low = split(lifted)
        full = dot(high, up_b_ref[0]) + dot(low, up_b_ref[0]) + dot(high, up_b_ref[1])
        space[0, l] = full[:extent, :extent] - full[extent:, extent:]
        space[1, l] = full[:extent, extent:] + full[extent:, :extent]

    for l in range(layers):
        pltpu.make_async_copy(pot_in.at[l], pot_in.at[l], pot_sem.at[l]).wait()
        local_pot = pot_in[l].reshape(extent, extent)
        field = jnp.concatenate([space[0, l] * local_pot, space[1, l] * local_pot], axis=1)
        fallen = dot(stacked(field, 1), down_b_ref[...])
        product = dot(down_a_ref[...], stacked(fallen, 0))
        swap = pltpu.roll(product[half:], half, 1)
        lane_half = lax.broadcasted_iota(jnp.int32, (half, 2 * half), 1)
        total = product[:half] + jnp.where(lane_half < half, swap, -swap)
        high, low = split(total)
        freq[l * half : (l + 1) * half, :] = jnp.concatenate([high, low], axis=1)

    def take_columns(d):
        number = ids_in[d].astype(jnp.int32)
        in_a = sub_half == number // half
        in_b = jnp.where(sub_half == number % half, 1.0, 0.0).astype(BF)
        none = jnp.zeros_like(in_b)
        upper_rows = jnp.concatenate([in_b, none], axis=1)
        lower_rows = jnp.concatenate([none, in_b], axis=1)
        picker = jnp.concatenate([upper_rows, lower_rows, upper_rows, lower_rows], axis=0)
        found = dot(freq[...], picker)
        rows = []
        for part in range(2):
            for l in range(layers):
                block = found[l * half : (l + 1) * half, part * LANES : (part + 1) * LANES]
                rows.append(jnp.sum(jnp.where(in_a, block, 0.0), axis=0, keepdims=True))
        if rows_msg > parts:
            rows.append(jnp.zeros((rows_msg - parts, LANES), F32))
        return jnp.concatenate(rows, axis=0)

    wide = 4
    rounds = count // wide

    def who(i):
        base = turned(rounds - 1 - i, 2) if width > 2 else me
        near = [peer(step) - me for step in range(wide - 1, -1, -1)]
        return [base + step for step in near]

    def give(other):
        pltpu.make_async_remote_copy(
            src_ref=back.at[other],
            dst_ref=back_in.at[me],
            send_sem=send_sem.at[3],
            recv_sem=recv_sem.at[3],
            device_id={"ga": other},
        ).start()

    def take_some(i, carry):
        @pl.when(i > 0)
        def _():
            for other in who(i - 1):
                give(other)

        tiles = [take_columns(d) for d in who(i)]
        for d, tile in zip(who(i), tiles):
            back[d] = tile
        return carry

    lax.fori_loop(0, rounds, take_some, 0)
    for other in who(rounds - 1)[:-1]:
        give(other)
    pltpu.make_async_copy(back.at[me], back_in.at[me], recv_sem.at[3]).start()
    load_last.wait()
    arrive(back_in, 3)

    final = dot(last_ref[...], stacked(back_in[...].reshape(count * rows_msg, LANES), 0))
    high, low = split(final)
    final_cat = jnp.concatenate([high, low], axis=1)
    place_rows = jnp.concatenate([place[...], place[...]], axis=0)
    spread_back = dot(final_cat, place_rows)
    for r in range(blocks):
        at_depth = sub_half == colrow[1, r : r + 1, :]
        span = slice(r * LANES, (r + 1) * LANES)
        k_row = kin[r : r + 1, :]
        for part in range(2):
            block = spread_back[part * half : (part + 1) * half, span]
            value = jnp.sum(jnp.where(at_depth, block, 0.0), axis=0, keepdims=True)
            applied_ref[part, r : r + 1, :] = value + k_row * orb[part, 0:1, span]

    rest.wait()
    tile_rows = 64
    owners = LANES // sub_rows
    spans = count // owners
    low = owners.bit_length() - 1
    ones = jnp.ones((16, LANES), BF)

    def tile_of(t):
        return lax.div(turned(spans - 1 - t, low), owners) if spans > 1 else lax.div(me, owners)

    def sweep(t, slot):
        for piece in range(LANES // tile_rows):
            start = tile_of(t) * LANES + piece * tile_rows
            at = pl.ds(pl.multiple_of(start, tile_rows), tile_rows)
            acc_re = jnp.zeros((tile_rows, LANES), F32)
            acc_im = jnp.zeros((tile_rows, LANES), F32)
            for r in range(blocks):
                span = slice(r * LANES, (r + 1) * LANES)
                a_re = applied_ref[0, r : r + 1, :]
                a_im = applied_ref[1, r : r + 1, :]
                o_re = orb[0, at, span]
                o_im = orb[1, at, span]
                acc_re = acc_re + (o_re * a_re + o_im * a_im)
                acc_im = acc_im + (o_re * a_im - o_im * a_re)
            rows = slice(piece * tile_rows, (piece + 1) * tile_rows)
            sums[slot, 0, rows, :] = acc_re
            sums[slot, 1, rows, :] = acc_im

    def narrow(t, slot):
        for part in range(2):
            high, low_part = split(sums[slot, part])
            line = dot(ones, high, NT) + dot(ones, low_part, NT)
            sub_out[t, part : part + 1, :] = line[0:1] * (1.0 / (slots * count))

    def share(t):
        base = turned(spans - 1 - t, low) if spans > 1 else me
        near = [peer(step) - me for step in range(owners - 1, -1, -1)]
        return [base + step for step in near]

    def publish(t, other):
        pltpu.make_async_remote_copy(
            src_ref=sub_out.at[t],
            dst_ref=sub_in.at[me],
            send_sem=send_sem.at[4],
            recv_sem=recv_sem.at[4],
            device_id={"ga": other},
        ).start()

    def sub_step(t, carry):
        narrow(t - 1, lax.rem(t - 1, 2))
        sweep(t, lax.rem(t, 2))
        for other in share(t - 1):
            publish(t - 1, other)
        return carry

    sweep(0, 0)
    lax.fori_loop(1, spans, sub_step, 0)
    narrow(spans - 1, (spans - 1) % 2)
    for other in share(spans - 1)[:-1]:
        publish(spans - 1, other)
    pltpu.make_async_copy(sub_out.at[spans - 1], sub_in.at[me], recv_sem.at[4]).start()
    arrive(sub_in, 4)
    total = jnp.sum(sub_in[...], axis=0)
    padded = jnp.concatenate([total, jnp.zeros((6, LANES), F32)], axis=0)
    offset = lax.rem(me, owners) * sub_rows
    mine = pltpu.roll(padded, lax.rem(LANES - offset, LANES), 1)
    sub_ref[...] = mine
    sent(ids_out, 0)
    sent(msg, 1)
    for l in range(layers):
        sent(pot_out.at[l], 2)
    sent(back, 3)
    sub_view = sub_in.at[pl.ds(0, count - 1)]
    pltpu.make_async_copy(sub_view, sub_view, send_sem.at[4]).wait()


def local(orbitals, coeff_cells, potential):
    count = lax.axis_size("ga")
    extent = potential.shape[1]
    layers = extent // count
    half = extent // 2
    bands_all, slots = orbitals.shape[1], orbitals.shape[2]
    blocks = slots // LANES
    parts = 2 * layers
    rows_msg = -(-parts // 8) * 8
    sub_rows = bands_all // count
    group = 8
    constants = [jnp.asarray(t) for t in tables(extent, count, rows_msg)]
    vmem = pl.BlockSpec(memory_space=pltpu.VMEM)
    staged = [(blocks, LANES), (layers, extent, extent)] + [t.shape for t in constants]
    kinds = [jnp.int32, F32] + [BF] * len(constants)
    scratch = [pltpu.VMEM(shape, kind) for shape, kind in zip(staged, kinds)] + [
        pltpu.VMEM((2, bands_all, slots), F32),
        pltpu.VMEM((4 * half + 16, slots), BF),
        pltpu.VMEM((LANES, slots), BF),
        pltpu.VMEM((count, 1, LANES), F32),
        pltpu.VMEM((count, 1, LANES), F32),
        pltpu.VMEM((count, rows_msg, LANES), F32),
        pltpu.VMEM((count, rows_msg, LANES), F32),
        pltpu.VMEM((layers, count, layers, LANES), F32),
        pltpu.VMEM((layers, count, layers, LANES), F32),
        pltpu.VMEM((2 * parts * half, group * LANES), BF),
        pltpu.VMEM((half, group * LANES), BF),
        pltpu.VMEM((2 * parts * half, half), F32),
        pltpu.VMEM((layers * half, 4 * half), BF),
        pltpu.VMEM((count, rows_msg, LANES), F32),
        pltpu.VMEM((count, rows_msg, LANES), F32),
        pltpu.VMEM((2, 2, LANES, LANES), F32),
        pltpu.VMEM((bands_all // LANES, 2, LANES), F32),
        pltpu.VMEM((count, 2, LANES), F32),
        pltpu.VMEM((blocks, LANES), F32),
        pltpu.VMEM((4, blocks, LANES), jnp.int32),
        pltpu.VMEM((2, layers, extent, extent), F32),
        pltpu.SemaphoreType.DMA,
        pltpu.SemaphoreType.DMA,
        pltpu.SemaphoreType.DMA((len(staged),)),
        pltpu.SemaphoreType.DMA((5,)),
        pltpu.SemaphoreType.DMA((5,)),
        pltpu.SemaphoreType.DMA((count // group,)),
        pltpu.SemaphoreType.DMA((count // group,)),
        pltpu.SemaphoreType.DMA((layers,)),
    ]
    applied, sub = pl.pallas_call(
        functools.partial(kernel, count, layers, extent, rows_msg, group),
        out_shape=(
            jax.ShapeDtypeStruct((2, blocks, LANES), F32),
            jax.ShapeDtypeStruct((8, LANES), F32),
        ),
        in_specs=[pl.BlockSpec(memory_space=pl.ANY)] * (3 + len(constants)),
        out_specs=(vmem, vmem),
        scratch_shapes=scratch,
        compiler_params=pltpu.CompilerParams(
            collective_id=0, has_side_effects=True, vmem_limit_bytes=60 * 1024 * 1024
        ),
    )(coeff_cells.reshape(blocks, LANES), potential, *constants, orbitals)
    applied = applied.reshape(2, 1, slots)
    subspace = jnp.transpose(sub[:2, :sub_rows])[:, :, None]
    return applied, subspace


def solution(mesh):
    in_specs = (P(None, "kpt", "ga"), P("ga"), P("ga", None, None))
    out_specs = (P(None, "kpt", "ga"), P("ga", None, "kpt"))
    return jax.shard_map(local, mesh=mesh, in_specs=in_specs, out_specs=out_specs, check_vma=False)
```

```python
import functools

import jax
import jax.numpy as jnp
import ml_dtypes
import numpy as np
from jax import lax
from jax.experimental import pallas as pl
from jax.experimental.pallas import tpu as pltpu
from jax.sharding import PartitionSpec as P

RADIUS = 30
BF = jnp.bfloat16
F32 = jnp.float32
LANES = 128
FINE = 16
NN = (((1,), (0,)), ((), ()))
NT = (((1,), (1,)), ((), ()))


def split_np(table):
    high = table.astype(np.float32).astype(ml_dtypes.bfloat16)
    low = (table - high.astype(np.float64)).astype(np.float32).astype(ml_dtypes.bfloat16)
    return high, low


def stack_np(table, axis):
    high, low = split_np(table)
    return np.concatenate([high, high, low], axis=axis)


def phases(extent, half):
    index = np.arange(half)
    freq = np.where(index < half // 2, index, index - half)
    angle = 2.0 * np.pi * ((np.arange(extent)[:, None] * freq[None, :]) % extent) / extent
    return np.cos(angle), np.sin(angle)


@functools.lru_cache(None)
def tables(extent, count, rows_msg):
    half = extent // 2
    layers = extent // count
    cos, sin = phases(extent, half)
    first = np.zeros((count, rows_msg, 2 * half))
    last = np.zeros((2 * half, count, rows_msg))
    for l in range(layers):
        z = np.arange(count) * layers + l
        first[:, l, :half], first[:, l, half:] = cos[z], -sin[z]
        first[:, layers + l, :half], first[:, layers + l, half:] = sin[z], cos[z]
        last[:half, :, l], last[:half, :, layers + l] = cos[z].T, sin[z].T
        last[half:, :, l], last[half:, :, layers + l] = -sin[z].T, cos[z].T
    first = first.reshape(count * rows_msg, 2 * half)
    last = last.reshape(2 * half, count * rows_msg) / float(extent) ** 3
    up_a = np.block([[cos, -sin], [sin, cos]])
    up_b = np.concatenate([cos.T, sin.T], axis=1)
    down_b = np.block([[cos, -sin], [sin, cos]])
    down_a = np.concatenate([cos.T, sin.T], axis=0)
    up_b_high, up_b_low = split_np(up_b)
    return (
        stack_np(first, 1),
        stack_np(up_a, 1),
        np.concatenate([up_b_high, up_b_high, up_b_low, np.zeros_like(up_b_low)]),
        stack_np(down_b, 0),
        stack_np(down_a, 1),
        stack_np(last, 1),
    )


def dot(left, right, dims=NN):
    return lax.dot_general(left, right, dims, preferred_element_type=F32)


def split(values):
    high = values.astype(BF)
    return high, (values - high.astype(F32)).astype(BF)


def stacked(values, axis):
    high, low = split(values)
    return jnp.concatenate([high, low, high], axis=axis)


def signed(values, extent):
    return jnp.where(values < extent // 2, values, values - extent)


def rows_iota(rows):
    return lax.broadcasted_iota(jnp.int32, (rows, LANES), 0).astype(F32).astype(BF)


def tall(row, rows):
    block = jnp.broadcast_to(row, (16, LANES)).astype(BF)
    return jnp.concatenate([block] * (rows // 16), axis=0)


def matches(index, row):
    return jnp.where(index == tall(row, index.shape[0]), BF(1.0), BF(0.0))


def bits_of(number, width):
    return [lax.rem(lax.div(number, 2**k), 2) for k in range(width)]


def kernel(
    count, layers, extent, rows_msg, group,
    cells_hbm, pot_hbm, first_hbm, up_a_hbm, up_b_hbm, down_b_hbm, down_a_hbm, last_hbm,
    orb_hbm, applied_ref, sub_ref,
    cells_ref, pot_ref, first_ref, up_a_ref, up_b_ref, down_b_ref, down_a_ref, last_ref,
    orb, place, ids_out, ids_in, msg, arrived, pot_out, pot_in,
    pick, fines, grid, mesh, back, back_in, sums, sub_out, sub_in, added, mixed, kin, colrow, space,
    win_sem, orb_sem, load_sem, send_sem, recv_sem, ids_sem, msg_sem, pot_sem,
):
    me = lax.axis_index("ga")
    half = extent // 2
    slots = orb.shape[2]
    blocks = slots // LANES
    bands_all = orb.shape[1]
    sub_rows = bands_all // count
    parts = 2 * layers
    batch = min(2, layers)
    folds = half // FINE
    width = count.bit_length() - 1
    turns = [(1 - 2 * bit) * 2**k for k, bit in enumerate(bits_of(me, width))]

    def peer(step):
        return me + sum([turns[k] for k in range(width) if step >> k & 1], 0)

    def turned(step, low):
        wide = width - low
        return me + sum([bit * turns[low + k] for k, bit in enumerate(bits_of(step, wide))], 0)

    far_first = [peer(step) for step in range(count - 1, 0, -1)]
    barrier = pltpu.get_barrier_semaphore()
    load_cells = pltpu.make_async_copy(cells_hbm, cells_ref, load_sem.at[0])
    load_cells.start()
    head = pltpu.make_async_copy(orb_hbm.at[:, 0:8, :], orb.at[:, 0:8, :], win_sem)
    head.start()
    for other in far_first:
        pl.semaphore_signal(barrier, inc=1, device_id={"ga": other})
    sources = (first_hbm, pot_hbm, up_a_hbm, up_b_hbm, down_b_hbm, down_a_hbm, last_hbm)
    targets = (first_ref, pot_ref, up_a_ref, up_b_ref, down_b_ref, down_a_ref, last_ref)
    loads = [
        pltpu.make_async_copy(source, target, load_sem.at[i + 1])
        for i, (source, target) in enumerate(zip(sources, targets))
    ]
    load_first, load_pot, load_up_a, load_up_b, load_down_b, load_down_a, load_last = loads
    for load in loads:
        load.start()
    rest = pltpu.make_async_copy(orb_hbm.at[:, 8:, :], orb.at[:, 8:, :], orb_sem)
    rest.start()
    groups = count // group
    my_group = me // group

    def exchange(source, target, phase, landed):
        own = pltpu.make_async_copy(source.at[me], target.at[me], landed)
        own.start()

        for other in far_first:
            pltpu.make_async_remote_copy(
                src_ref=source.at[other],
                dst_ref=target.at[me],
                send_sem=send_sem.at[phase],
                recv_sem=landed,
                device_id={"ga": other},
            ).start()

    def arrive(target, phase):
        pltpu.make_async_copy(target, target, recv_sem.at[phase]).wait()

    def sent(source, phase):
        view = source.at[pl.ds(0, count - 1)]
        pltpu.make_async_copy(view, view, send_sem.at[phase]).wait()

    load_cells.wait()
    cells = cells_ref[...]
    live = cells >= 0
    column = jnp.right_shift(cells, extent.bit_length() - 1)
    rolled = pltpu.roll(column, 1, 1)
    lane = lax.broadcasted_iota(jnp.int32, cells.shape, 1)
    row = lax.broadcasted_iota(jnp.int32, cells.shape, 0)
    earlier = jnp.where(lane == 0, pltpu.roll(rolled, 1, 0), rolled)
    earlier = jnp.where((lane == 0) & (row == 0), -1, earlier)
    starts = live & (column != earlier)
    flags = starts.astype(F32).astype(BF)
    sq = lambda axis: lax.broadcasted_iota(jnp.int32, (LANES, LANES), axis)
    upper = (sq(0) <= sq(1)).astype(F32).astype(BF)
    inner = dot(flags, upper)
    totals = dot(flags, jnp.ones((LANES, LANES), BF))
    below = lax.broadcasted_iota(jnp.int32, (blocks, blocks), 1) < lax.broadcasted_iota(
        jnp.int32, (blocks, blocks), 0
    )
    outer = dot(below.astype(F32).astype(BF), totals.astype(BF))
    local = (inner + outer - 1.0).astype(jnp.int32)
    local = jnp.where(live, local, -1)
    safe = jnp.where(live, cells, 0)
    plane_c = safe % extent
    plane_b = safe // extent % extent
    plane_a = safe // (extent * extent)
    fa, fb, fc = signed(plane_a, extent), signed(plane_b, extent), signed(plane_c, extent)
    kinetic = (fa * fa + fb * fb + fc * fc).astype(F32) / (RADIUS * RADIUS)
    kin[...] = jnp.where(live, kinetic, 0.0)
    small_a = plane_a % half
    colrow[0] = local.astype(F32)
    colrow[1] = (plane_c % half).astype(F32)
    colrow[2] = jnp.where(starts, small_a % FINE, 0).astype(F32)
    colrow[3] = jnp.where(starts, small_a // FINE * half + plane_b % half, 0).astype(F32)

    head.wait()
    deep = rows_iota(half)
    full = rows_iota(LANES)
    sub_ids = lax.broadcasted_iota(jnp.int32, (16, LANES), 0)
    chunk = 4
    sticks = jnp.zeros((4 * half + 16, LANES), F32)
    for c in range(blocks // chunk):
        pieces = []
        for r in range(c * chunk, (c + 1) * chunk):
            span = slice(r * LANES, (r + 1) * LANES)
            at_depth = matches(deep, colrow[1, r : r + 1, :])
            lines = []
            for part in range(2):
                for value in split(orb[part, 0:1, span]):
                    lines.append(at_depth * tall(value.astype(F32), half))
            is_fine, is_wide = colrow[2, r : r + 1, :], colrow[3, r : r + 1, :]
            tail = jnp.where(sub_ids == 0, is_fine, jnp.where(sub_ids == 1, is_wide, 0.0))
            pieces.append(jnp.concatenate(lines + [tail.astype(BF)], axis=0))
            place[:, span] = matches(full, colrow[0, r : r + 1, :])
        span = slice(c * chunk * LANES, (c + 1) * chunk * LANES)
        sticks = sticks + dot(jnp.concatenate(pieces, axis=1), place[:, span], NT)
    code = sticks[4 * half : 4 * half + 1] * (folds * half) + sticks[4 * half + 1 : 4 * half + 2]

    def copy_ids(d, carry):
        ids_out[d] = code
        return carry

    lax.fori_loop(0, count, copy_ids, 0)
    both = jnp.concatenate(
        [
            sticks[0:half] + sticks[half : 2 * half],
            sticks[2 * half : 3 * half] + sticks[3 * half : 4 * half],
        ],
        axis=0,
    )
    load_first.wait()
    msg[...] = dot(first_ref[...], stacked(both, 0)).reshape(count, rows_msg, LANES)
    pl.semaphore_wait(barrier, count - 1)
    exchange(ids_out, ids_in, 0, ids_sem.at[my_group])
    exchange(msg, arrived, 1, msg_sem.at[my_group])

    load_pot.wait()
    for a in range(layers):
        across = jnp.transpose(pot_ref[a])
        for d in range(count):
            for l in range(layers):
                row = l % batch * layers + a
                pot_out[l // batch, d, row : row + 1, :] = across[d * layers + l : d * layers + l + 1]
    for c in range(layers // batch):
        exchange(pot_out.at[c], pot_in.at[c], 2, pot_sem.at[c])

    grid[...] = jnp.zeros_like(grid)
    broad = rows_iota(folds * half)

    def gather_group(step, carry):
        g = lax.div(turned(step, group.bit_length() - 1), group)
        ids_view = ids_in.at[pl.ds(g * group, group)]
        pltpu.make_async_copy(ids_view, ids_view, ids_sem.at[g]).wait()
        msg_view = arrived.at[pl.ds(g * group, group)]
        pltpu.make_async_copy(msg_view, msg_view, msg_sem.at[g]).wait()
        pieces = []
        for k in range(group):
            d = g * group + k
            code = ids_in[d]
            is_fine = jnp.floor(code * (1.0 / (folds * half)))
            fines[d] = is_fine
            span = pl.ds(pl.multiple_of(d * LANES, LANES), LANES)
            pick[:, span] = matches(broad, code - is_fine * (folds * half))
            high, low = split(arrived[d])
            high, low = high.astype(F32), low.astype(F32)
            here = jnp.broadcast_to(is_fine, (rows_msg, LANES))
            lines = [jnp.where(here == f, high, 0.0) for f in range(FINE)]
            lines += [jnp.where(here == f, low, 0.0) for f in range(FINE)]
            pieces.append(jnp.concatenate(lines, axis=0).astype(BF))
        span = pl.ds(pl.multiple_of(g * group * LANES, group * LANES), group * LANES)
        grid[...] += dot(jnp.concatenate(pieces, axis=1), pick[:, span], NT)
        return carry

    lax.fori_loop(0, groups, gather_group, 0)
    load_up_a.wait()
    load_up_b.wait()
    load_down_b.wait()
    load_down_a.wait()

    rows_mesh = FINE * rows_msg
    halves = folds * half // LANES
    per = LANES // half
    both = grid[0:rows_mesh] + grid[rows_mesh:]
    for h in range(halves):
        mesh[h] = both[:, h * LANES : (h + 1) * LANES]

    lines = []
    for part in range(2):
        for h in range(halves):
            blocks_of = [
                mesh[h, pl.ds(part * layers + l, FINE, stride=rows_msg), :] for l in range(layers)
            ]
            for q in range(per):
                lines.append(
                    jnp.concatenate([block[:, q * half : (q + 1) * half] for block in blocks_of], axis=1)
                )
    lifted = dot(up_a_ref[...], stacked(jnp.concatenate(lines, axis=0), 0))
    for l in range(layers):
        plane = lifted[:, l * half : (l + 1) * half]
        high = plane.astype(BF).astype(F32)
        pair = jnp.concatenate([high, plane - high], axis=1).astype(BF)
        whole = dot(jnp.concatenate([pair, pair], axis=1), up_b_ref[...])
        space[0, l] = whole[:extent, :extent] - whole[extent:, extent:]
        space[1, l] = whole[:extent, extent:] + whole[extent:, :extent]

    mesh[...] = jnp.zeros_like(mesh)
    lane_half = lax.broadcasted_iota(jnp.int32, (half, 2 * half), 1)
    for c in range(layers // batch):
        pltpu.make_async_copy(pot_in.at[c], pot_in.at[c], pot_sem.at[c]).wait()
        fallen = []
        for i in range(batch):
            l = c * batch + i
            local_pot = pot_in[c, :, i * layers : (i + 1) * layers, :].reshape(extent, extent)
            field = jnp.concatenate([space[0, l] * local_pot, space[1, l] * local_pot], axis=1)
            fallen.append(dot(stacked(field, 1), down_b_ref[...]))
        products = dot(down_a_ref[...], stacked(jnp.concatenate(fallen, axis=1), 0))
        for i in range(batch):
            product = products[:, i * 2 * half : (i + 1) * 2 * half]
            swap = pltpu.roll(product[half:], half, 1)
            total = product[:half] + jnp.where(lane_half < half, swap, -swap)
            for part in range(2):
                block = total[:, part * half : (part + 1) * half]
                for h in range(halves):
                    sides = [block[q * FINE : (q + 1) * FINE] for q in range(h * per, (h + 1) * per)]
                    line = jnp.concatenate(sides, axis=1)
                    at = part * layers + c * batch + i
                    mesh[h, pl.ds(at, FINE, stride=rows_msg), :] = line

    wide = 4
    rounds = count // wide
    left = jnp.concatenate(split(jnp.concatenate([mesh[h] for h in range(halves)], axis=1)), axis=0)

    def give(other):
        pltpu.make_async_remote_copy(
            src_ref=back.at[other],
            dst_ref=back_in.at[me],
            send_sem=send_sem.at[3],
            recv_sem=recv_sem.at[3],
            device_id={"ga": other},
        ).start()

    def first_of(i):
        return lax.div(peer((rounds - 1 - i) * wide), wide) * wide

    def find(i):
        span = pl.ds(pl.multiple_of(first_of(i) * LANES, wide * LANES), wide * LANES)
        return dot(left, pick[:, span])

    found = find(0)
    for i in range(rounds):
        following = find(i + 1) if i + 1 < rounds else None
        for k in range(wide):
            here = jnp.broadcast_to(fines[first_of(i) + k], (rows_msg, LANES))
            tile = jnp.zeros((rows_msg, LANES), F32)
            for f in range(FINE):
                cut = (slice(f * rows_msg, (f + 1) * rows_msg), slice(k * LANES, (k + 1) * LANES))
                tile = tile + jnp.where(here == f, found[:rows_mesh][cut] + found[rows_mesh:][cut], 0.0)
            back[first_of(i) + k] = tile
        if i > 0:
            for step in range(wide):
                give(peer((rounds - i) * wide + wide - 1 - step))
        found = following
    for step in range(wide - 1):
        give(peer(wide - 1 - step))
    pltpu.make_async_copy(back.at[me], back_in.at[me], recv_sem.at[3]).start()
    rest.wait()

    def add(t, carry):
        at = pl.ds(pl.multiple_of(t * 16, 16), 16)
        added[at, :] = orb[0, at, :] + orb[1, at, :]
        return carry

    lax.fori_loop(0, bands_all // 16, add, 0)
    load_last.wait()
    arrive(back_in, 3)

    sub_half = lax.broadcasted_iota(jnp.int32, (half, LANES), 0).astype(F32)
    final = dot(last_ref[...], stacked(back_in[...].reshape(count * rows_msg, LANES), 0))
    high, low = split(final)
    final_cat = jnp.concatenate([high, low], axis=1)
    place_rows = jnp.concatenate([place[...], place[...]], axis=0)
    spread_back = dot(final_cat, place_rows)
    for r in range(blocks):
        at_depth = sub_half == colrow[1, r : r + 1, :]
        span = slice(r * LANES, (r + 1) * LANES)
        k_row = kin[r : r + 1, :]
        for part in range(2):
            block = spread_back[part * half : (part + 1) * half, span]
            value = jnp.sum(jnp.where(at_depth, block, 0.0), axis=0, keepdims=True)
            applied_ref[part, r : r + 1, :] = value + k_row * orb[part, 0:1, span]

    u, v = applied_ref[0], applied_ref[1]
    mixed[0], mixed[1], mixed[2] = u, u - v, u + v
    tile_rows = 64
    owners = tile_rows // sub_rows
    spans = count // owners
    low = owners.bit_length() - 1

    def tile_of(t):
        return lax.div(turned(spans - 1 - t, low), owners) if spans > 1 else lax.div(me, owners)

    def sweep(t, slot):
        at = pl.ds(pl.multiple_of(tile_of(t) * tile_rows, tile_rows), tile_rows)
        acc = [jnp.zeros((tile_rows, LANES), F32) for _ in range(3)]
        for r in range(blocks):
            span = slice(r * LANES, (r + 1) * LANES)
            acc[0] = acc[0] + added[at, span] * mixed[0, r : r + 1, :]
            acc[1] = acc[1] + orb[1, at, span] * mixed[1, r : r + 1, :]
            acc[2] = acc[2] + orb[0, at, span] * mixed[2, r : r + 1, :]
        sums[slot, 0] = acc[0] - acc[1]
        sums[slot, 1] = acc[2] - acc[0]

    def narrow(t, slot):
        both = sums[slot].reshape(2 * tile_rows, LANES)
        line = jnp.sum(jnp.transpose(both), axis=0, keepdims=True)
        sub_out[t] = line * (1.0 / (slots * count))

    def share(t):
        base = turned(spans - 1 - t, low) if spans > 1 else me
        near = [peer(step) - me for step in range(owners - 1, -1, -1)]
        return [base + step for step in near]

    def publish(t, other):
        pltpu.make_async_remote_copy(
            src_ref=sub_out.at[t],
            dst_ref=sub_in.at[me],
            send_sem=send_sem.at[4],
            recv_sem=recv_sem.at[4],
            device_id={"ga": other},
        ).start()

    def sub_step(t, carry):
        narrow(t - 1, lax.rem(t - 1, 2))
        sweep(t, lax.rem(t, 2))
        for other in share(t - 1):
            publish(t - 1, other)
        return carry

    sweep(0, 0)
    lax.fori_loop(1, spans, sub_step, 0)
    narrow(spans - 1, (spans - 1) % 2)
    for other in share(spans - 1)[:-1]:
        publish(spans - 1, other)
    pltpu.make_async_copy(sub_out.at[spans - 1], sub_in.at[me], recv_sem.at[4]).start()
    arrive(sub_in, 4)
    total = jnp.broadcast_to(jnp.sum(sub_in[...], axis=0), (8, LANES))
    offset = lax.rem(me, owners) * sub_rows
    mine = pltpu.roll(total, lax.rem(LANES - offset, LANES), 1)
    sub_ref[0] = mine[0:1, :sub_rows]
    sub_ref[1] = mine[0:1, tile_rows : tile_rows + sub_rows]
    sent(ids_out, 0)
    sent(msg, 1)
    for c in range(layers // batch):
        sent(pot_out.at[c], 2)
    sent(back, 3)
    sub_view = sub_in.at[pl.ds(0, count - 1)]
    pltpu.make_async_copy(sub_view, sub_view, send_sem.at[4]).wait()


def emit(applied_ref, sub_ref, applied_out, sub_out):
    applied_out[...] = applied_ref[...]
    sub_out[...] = sub_ref[...]


def local(orbitals, coeff_cells, potential):
    count = lax.axis_size("ga")
    extent = potential.shape[1]
    layers = extent // count
    half = extent // 2
    bands_all, slots = orbitals.shape[1], orbitals.shape[2]
    blocks = slots // LANES
    parts = 2 * layers
    rows_msg = -(-parts // 8) * 8
    sub_rows = bands_all // count
    group = 8
    batch = min(2, layers)
    folds = half // FINE
    constants = [jnp.asarray(t) for t in tables(extent, count, rows_msg)]
    vmem = pl.BlockSpec(memory_space=pltpu.VMEM)
    staged = [(blocks, LANES), (layers, extent, extent)] + [t.shape for t in constants]
    kinds = [jnp.int32, F32] + [BF] * len(constants)
    scratch = [pltpu.VMEM(shape, kind) for shape, kind in zip(staged, kinds)] + [
        pltpu.VMEM((2, bands_all, slots), F32),
        pltpu.VMEM((LANES, slots), BF),
        pltpu.VMEM((count, 1, LANES), F32),
        pltpu.VMEM((count, 1, LANES), F32),
        pltpu.VMEM((count, rows_msg, LANES), F32),
        pltpu.VMEM((count, rows_msg, LANES), F32),
        pltpu.VMEM((layers // batch, count, batch * layers, LANES), F32),
        pltpu.VMEM((layers // batch, count, batch * layers, LANES), F32),
        pltpu.VMEM((folds * half, count * LANES), BF),
        pltpu.VMEM((count, 1, LANES), F32),
        pltpu.VMEM((2 * FINE * rows_msg, folds * half), F32),
        pltpu.VMEM((folds * half // LANES, FINE * rows_msg, LANES), F32),
        pltpu.VMEM((count, rows_msg, LANES), F32),
        pltpu.VMEM((count, rows_msg, LANES), F32),
        pltpu.VMEM((2, 2, 64, LANES), F32),
        pltpu.VMEM((bands_all // 64, 1, LANES), F32),
        pltpu.VMEM((count, 1, LANES), F32),
        pltpu.VMEM((bands_all, slots), F32),
        pltpu.VMEM((3, blocks, LANES), F32),
        pltpu.VMEM((blocks, LANES), F32),
        pltpu.VMEM((4, blocks, LANES), F32),
        pltpu.VMEM((2, layers, extent, extent), F32),
        pltpu.SemaphoreType.DMA,
        pltpu.SemaphoreType.DMA,
        pltpu.SemaphoreType.DMA((len(staged),)),
        pltpu.SemaphoreType.DMA((5,)),
        pltpu.SemaphoreType.DMA((5,)),
        pltpu.SemaphoreType.DMA((count // group,)),
        pltpu.SemaphoreType.DMA((count // group,)),
        pltpu.SemaphoreType.DMA((layers // batch,)),
    ]
    applied, sub = pl.pallas_call(
        functools.partial(kernel, count, layers, extent, rows_msg, group),
        out_shape=(
            pltpu.VMEM((2, blocks, LANES), F32),
            pltpu.VMEM((2, 1, sub_rows), F32),
        ),
        in_specs=[pl.BlockSpec(memory_space=pl.ANY)] * (3 + len(constants)),
        out_specs=(vmem, vmem),
        scratch_shapes=scratch,
        compiler_params=pltpu.CompilerParams(
            collective_id=0, has_side_effects=True, vmem_limit_bytes=60 * 1024 * 1024
        ),
    )(coeff_cells.reshape(blocks, LANES), potential, *constants, orbitals)
    applied, sub = pl.pallas_call(
        emit,
        out_shape=(
            jax.ShapeDtypeStruct(applied.shape, F32),
            jax.ShapeDtypeStruct(sub.shape, F32),
        ),
        in_specs=[vmem, vmem],
        out_specs=(vmem, vmem),
        compiler_params=pltpu.CompilerParams(vmem_limit_bytes=1024 * 1024),
    )(applied, sub)
    applied = applied.reshape(2, 1, slots)
    subspace = jnp.transpose(sub, (2, 0, 1))
    return applied, subspace


def solution(mesh):
    in_specs = (P(None, "kpt", "ga"), P("ga"), P("ga", None, None))
    out_specs = (P(None, "kpt", "ga"), P("ga", None, "kpt"))
    return jax.shard_map(local, mesh=mesh, in_specs=in_specs, out_specs=out_specs, check_vma=False)
```

```python
import functools

import jax
import jax.numpy as jnp
import ml_dtypes
import numpy as np
from jax import lax
from jax.experimental import pallas as pl
from jax.experimental.pallas import tpu as pltpu
from jax.sharding import PartitionSpec as P

RADIUS = 30
BF = jnp.bfloat16
F32 = jnp.float32
LANES = 128
FINE = 16
NN = (((1,), (0,)), ((), ()))
NT = (((1,), (1,)), ((), ()))


def split_np(table):
    high = table.astype(np.float32).astype(ml_dtypes.bfloat16)
    low = (table - high.astype(np.float64)).astype(np.float32).astype(ml_dtypes.bfloat16)
    return high, low


def stack_np(table, axis):
    high, low = split_np(table)
    return np.concatenate([high, high, low], axis=axis)


def phases(extent, half):
    index = np.arange(half)
    freq = np.where(index < half // 2, index, index - half)
    angle = 2.0 * np.pi * ((np.arange(extent)[:, None] * freq[None, :]) % extent) / extent
    return np.cos(angle), np.sin(angle)


@functools.lru_cache(None)
def tables(extent, count, rows_msg):
    half = extent // 2
    layers = extent // count
    cos, sin = phases(extent, half)
    first = np.zeros((count, rows_msg, 2 * half))
    last = np.zeros((2 * half, count, rows_msg))
    for l in range(layers):
        z = np.arange(count) * layers + l
        first[:, l, :half], first[:, l, half:] = cos[z], -sin[z]
        first[:, layers + l, :half], first[:, layers + l, half:] = sin[z], cos[z]
        last[:half, :, l], last[:half, :, layers + l] = cos[z].T, sin[z].T
        last[half:, :, l], last[half:, :, layers + l] = -sin[z].T, cos[z].T
    first = first.reshape(count * rows_msg, 2 * half)
    last = last.reshape(2 * half, count * rows_msg) / float(extent) ** 3
    up_a = np.block([[cos, -sin], [sin, cos]])
    up_b = np.concatenate([cos.T, sin.T], axis=1)
    down_b = np.block([[cos, -sin], [sin, cos]])
    down_a = np.concatenate([cos.T, sin.T], axis=0)
    up_b_high, up_b_low = split_np(up_b)
    return (
        stack_np(first, 1),
        stack_np(up_a, 1),
        np.concatenate([up_b_high, up_b_high, up_b_low, np.zeros_like(up_b_low)]),
        stack_np(down_b, 0),
        stack_np(down_a, 1),
        stack_np(last, 1),
    )


def sheared(values, shifts):
    row = lax.broadcasted_iota(jnp.int32, values.shape, 0) % 4
    turned = [pltpu.roll(values, shift, 1) for shift in shifts]
    return jnp.where(row == 0, turned[0], jnp.where(row == 1, turned[1], turned[2]))


def most_columns(extent, count):
    index = np.arange(extent)
    square = np.where(index < extent // 2, index, index - extent) ** 2
    return -(-int((square[:, None] + square[None, :] <= RADIUS * RADIUS).sum()) // count)


def is_narrow(extent, count, parts):
    return parts == 8 and most_columns(extent, count) <= 3 * (LANES // 4)


def dot(left, right, dims=NN):
    return lax.dot_general(left, right, dims, preferred_element_type=F32)


def split(values):
    high = values.astype(BF)
    return high, (values - high.astype(F32)).astype(BF)


def stacked(values, axis):
    high, low = split(values)
    return jnp.concatenate([high, low, high], axis=axis)


def signed(values, extent):
    return jnp.where(values < extent // 2, values, values - extent)


def rows_iota(rows):
    return lax.broadcasted_iota(jnp.int32, (rows, LANES), 0).astype(F32).astype(BF)


def tall(row, rows):
    block = jnp.broadcast_to(row, (16, LANES)).astype(BF)
    return jnp.concatenate([block] * (rows // 16), axis=0)


def matches(index, row):
    return jnp.where(index == tall(row, index.shape[0]), BF(1.0), BF(0.0))


def bits_of(number, width):
    return [lax.rem(lax.div(number, 2**k), 2) for k in range(width)]


def kernel(
    count, layers, extent, rows_msg, group,
    cells_hbm, pot_hbm, first_hbm, up_a_hbm, up_b_hbm, down_b_hbm, down_a_hbm, last_hbm,
    orb_hbm, applied_ref, sub_ref,
    cells_ref, pot_ref, first_ref, up_a_ref, up_b_ref, down_b_ref, down_a_ref, last_ref,
    orb, place, ids_out, ids_in, msg, arrived, pot_out, pot_in,
    pick, fines, grid, mesh, back, back_in, sums, sub_out, sub_in, added, mixed, kin, colrow, space,
    win_sem, orb_sem, load_sem, send_sem, recv_sem, ids_sem, msg_sem, pot_sem,
):
    me = lax.axis_index("ga")
    half = extent // 2
    slots = orb.shape[2]
    blocks = slots // LANES
    bands_all = orb.shape[1]
    sub_rows = bands_all // count
    parts = 2 * layers
    batch = min(2, layers)
    folds = half // FINE
    narrow_msg = is_narrow(extent, count, parts)
    room = 3 * (LANES // 4)
    width = count.bit_length() - 1
    turns = [(1 - 2 * bit) * 2**k for k, bit in enumerate(bits_of(me, width))]

    def peer(step):
        return me + sum([turns[k] for k in range(width) if step >> k & 1], 0)

    def turned(step, low):
        wide = width - low
        return me + sum([bit * turns[low + k] for k, bit in enumerate(bits_of(step, wide))], 0)

    far_first = [peer(step) for step in range(count - 1, 0, -1)]
    barrier = pltpu.get_barrier_semaphore()
    load_cells = pltpu.make_async_copy(cells_hbm, cells_ref, load_sem.at[0])
    load_cells.start()
    head = pltpu.make_async_copy(orb_hbm.at[:, 0:8, :], orb.at[:, 0:8, :], win_sem)
    head.start()
    for other in far_first:
        pl.semaphore_signal(barrier, inc=1, device_id={"ga": other})
    sources = (first_hbm, pot_hbm, up_a_hbm, up_b_hbm, down_b_hbm, down_a_hbm, last_hbm)
    targets = (first_ref, pot_ref, up_a_ref, up_b_ref, down_b_ref, down_a_ref, last_ref)
    loads = [
        pltpu.make_async_copy(source, target, load_sem.at[i + 1])
        for i, (source, target) in enumerate(zip(sources, targets))
    ]
    load_first, load_pot, load_up_a, load_up_b, load_down_b, load_down_a, load_last = loads
    for load in loads:
        load.start()
    rest = pltpu.make_async_copy(orb_hbm.at[:, 8:, :], orb.at[:, 8:, :], orb_sem)
    rest.start()
    groups = count // group
    my_group = me // group

    def exchange(source, target, phase, landed):
        own = pltpu.make_async_copy(source.at[me], target.at[me], landed)
        own.start()

        for other in far_first:
            pltpu.make_async_remote_copy(
                src_ref=source.at[other],
                dst_ref=target.at[me],
                send_sem=send_sem.at[phase],
                recv_sem=landed,
                device_id={"ga": other},
            ).start()

    def arrive(target, phase):
        pltpu.make_async_copy(target, target, recv_sem.at[phase]).wait()

    def sent(source, phase):
        view = source.at[pl.ds(0, count - 1)]
        pltpu.make_async_copy(view, view, send_sem.at[phase]).wait()

    load_cells.wait()
    cells = cells_ref[...]
    live = cells >= 0
    column = jnp.right_shift(cells, extent.bit_length() - 1)
    rolled = pltpu.roll(column, 1, 1)
    lane = lax.broadcasted_iota(jnp.int32, cells.shape, 1)
    row = lax.broadcasted_iota(jnp.int32, cells.shape, 0)
    earlier = jnp.where(lane == 0, pltpu.roll(rolled, 1, 0), rolled)
    earlier = jnp.where((lane == 0) & (row == 0), -1, earlier)
    starts = live & (column != earlier)
    flags = starts.astype(F32).astype(BF)
    sq = lambda axis: lax.broadcasted_iota(jnp.int32, (LANES, LANES), axis)
    upper = (sq(0) <= sq(1)).astype(F32).astype(BF)
    inner = dot(flags, upper)
    totals = dot(flags, jnp.ones((LANES, LANES), BF))
    below = lax.broadcasted_iota(jnp.int32, (blocks, blocks), 1) < lax.broadcasted_iota(
        jnp.int32, (blocks, blocks), 0
    )
    outer = dot(below.astype(F32).astype(BF), totals.astype(BF))
    local = (inner + outer - 1.0).astype(jnp.int32)
    local = jnp.where(live, local, -1)
    safe = jnp.where(live, cells, 0)
    plane_c = safe % extent
    plane_b = safe // extent % extent
    plane_a = safe // (extent * extent)
    fa, fb, fc = signed(plane_a, extent), signed(plane_b, extent), signed(plane_c, extent)
    kinetic = (fa * fa + fb * fb + fc * fc).astype(F32) / (RADIUS * RADIUS)
    kin[...] = jnp.where(live, kinetic, 0.0)
    small_a = plane_a % half
    colrow[0] = local.astype(F32)
    colrow[1] = (plane_c % half).astype(F32)
    colrow[2] = jnp.where(starts, small_a % FINE, 0).astype(F32)
    colrow[3] = jnp.where(starts, small_a // FINE * half + plane_b % half, 0).astype(F32)

    head.wait()
    deep = rows_iota(half)
    full = rows_iota(LANES)
    sub_ids = lax.broadcasted_iota(jnp.int32, (16, LANES), 0)
    chunk = 4
    sticks = jnp.zeros((4 * half + 16, LANES), F32)
    for c in range(blocks // chunk):
        pieces = []
        for r in range(c * chunk, (c + 1) * chunk):
            span = slice(r * LANES, (r + 1) * LANES)
            at_depth = matches(deep, colrow[1, r : r + 1, :])
            lines = []
            for part in range(2):
                for value in split(orb[part, 0:1, span]):
                    lines.append(at_depth * tall(value.astype(F32), half))
            is_fine, is_wide = colrow[2, r : r + 1, :], colrow[3, r : r + 1, :]
            tail = jnp.where(sub_ids == 0, is_fine, jnp.where(sub_ids == 1, is_wide, 0.0))
            pieces.append(jnp.concatenate(lines + [tail.astype(BF)], axis=0))
            place[:, span] = matches(full, colrow[0, r : r + 1, :])
        span = slice(c * chunk * LANES, (c + 1) * chunk * LANES)
        sticks = sticks + dot(jnp.concatenate(pieces, axis=1), place[:, span], NT)
    code = sticks[4 * half : 4 * half + 1] * (folds * half) + sticks[4 * half + 1 : 4 * half + 2]

    both = jnp.concatenate(
        [
            sticks[0:half] + sticks[half : 2 * half],
            sticks[2 * half : 3 * half] + sticks[3 * half : 4 * half],
        ],
        axis=0,
    )
    load_first.wait()
    sheet = dot(first_ref[...], stacked(both, 0)).reshape(count, rows_msg, LANES)
    if narrow_msg:
        row_of = lax.broadcasted_iota(jnp.int32, (count, rows_msg, LANES), 1)
        lane_of = lax.broadcasted_iota(jnp.int32, (count, rows_msg, LANES), 2)
        ends = jnp.where(row_of < 4, sheet[:, rows_msg - 1 : rows_msg, :], code[None])
        ends = ends.reshape(count * rows_msg, LANES)
        ends = sheared(ends, [room, room - LANES // 4, room - LANES // 2])
        sheet = jnp.where(lane_of < room, sheet, ends.reshape(count, rows_msg, LANES))
        msg[...] = sheet[:, : rows_msg - 1, :]
    else:
        msg[...] = sheet
        ids_out[...] = jnp.broadcast_to(code[None], ids_out.shape)
    pl.semaphore_wait(barrier, count - 1)
    if not narrow_msg:
        exchange(ids_out, ids_in, 0, ids_sem.at[my_group])
    exchange(msg, arrived, 1, msg_sem.at[my_group])

    load_pot.wait()
    for a in range(layers):
        across = jnp.transpose(pot_ref[a])
        for d in range(count):
            for l in range(layers):
                row = l % batch * layers + a
                pot_out[l // batch, d, row : row + 1, :] = across[d * layers + l : d * layers + l + 1]
    for c in range(layers // batch):
        exchange(pot_out.at[c], pot_in.at[c], 2, pot_sem.at[c])

    grid[...] = jnp.zeros_like(grid)
    broad = rows_iota(folds * half)
    row_of = lax.broadcasted_iota(jnp.int32, (rows_msg, LANES), 0)
    lane_of = lax.broadcasted_iota(jnp.int32, (rows_msg, LANES), 1)

    def gather_group(step, carry):
        g = lax.div(turned(step, group.bit_length() - 1), group)
        if not narrow_msg:
            ids_view = ids_in.at[pl.ds(g * group, group)]
            pltpu.make_async_copy(ids_view, ids_view, ids_sem.at[g]).wait()
        msg_view = arrived.at[pl.ds(g * group, group)]
        pltpu.make_async_copy(msg_view, msg_view, msg_sem.at[g]).wait()
        pieces = []
        for k in range(group):
            d = g * group + k
            tile = arrived[d]
            if narrow_msg:
                tile = jnp.concatenate([tile, tile[0:1]], axis=0)
                ends = sheared(tile, [LANES // 4, LANES // 2, room])
                ends = jnp.where(lane_of // (LANES // 4) == row_of % 4, ends, 0.0)
                ends = jnp.where(row_of % 4 < 3, ends, 0.0)
                final_row = ends[0:1] + ends[1:2] + ends[2:3]
                code = ends[4:5] + ends[5:6] + ends[6:7]
                tile = jnp.where(row_of == rows_msg - 1, final_row, tile)
                tile = jnp.where(lane_of < room, tile, 0.0)
            else:
                code = ids_in[d]
            is_fine = jnp.floor(code * (1.0 / (folds * half)))
            fines[d] = is_fine
            span = pl.ds(pl.multiple_of(d * LANES, LANES), LANES)
            pick[:, span] = matches(broad, code - is_fine * (folds * half))
            high, low = split(tile)
            high, low = high.astype(F32), low.astype(F32)
            here = jnp.broadcast_to(is_fine, (rows_msg, LANES))
            lines = [jnp.where(here == f, high, 0.0) for f in range(FINE)]
            lines += [jnp.where(here == f, low, 0.0) for f in range(FINE)]
            pieces.append(jnp.concatenate(lines, axis=0).astype(BF))
        span = pl.ds(pl.multiple_of(g * group * LANES, group * LANES), group * LANES)
        grid[...] += dot(jnp.concatenate(pieces, axis=1), pick[:, span], NT)
        return carry

    lax.fori_loop(0, groups, gather_group, 0)
    load_up_a.wait()
    load_up_b.wait()
    load_down_b.wait()
    load_down_a.wait()

    rows_mesh = FINE * rows_msg
    halves = folds * half // LANES
    per = LANES // half
    both = grid[0:rows_mesh] + grid[rows_mesh:]
    for h in range(halves):
        mesh[h] = both[:, h * LANES : (h + 1) * LANES]

    lines = []
    for part in range(2):
        for h in range(halves):
            blocks_of = [
                mesh[h, pl.ds(part * layers + l, FINE, stride=rows_msg), :] for l in range(layers)
            ]
            for q in range(per):
                lines.append(
                    jnp.concatenate([block[:, q * half : (q + 1) * half] for block in blocks_of], axis=1)
                )
    lifted = dot(up_a_ref[...], stacked(jnp.concatenate(lines, axis=0), 0))
    for l in range(layers):
        plane = lifted[:, l * half : (l + 1) * half]
        high = plane.astype(BF).astype(F32)
        pair = jnp.concatenate([high, plane - high], axis=1).astype(BF)
        whole = dot(jnp.concatenate([pair, pair], axis=1), up_b_ref[...])
        space[0, l] = whole[:extent, :extent] - whole[extent:, extent:]
        space[1, l] = whole[:extent, extent:] + whole[extent:, :extent]

    mesh[...] = jnp.zeros_like(mesh)
    lane_half = lax.broadcasted_iota(jnp.int32, (half, 2 * half), 1)
    for c in range(layers // batch):
        pltpu.make_async_copy(pot_in.at[c], pot_in.at[c], pot_sem.at[c]).wait()
        fallen = []
        for i in range(batch):
            l = c * batch + i
            local_pot = pot_in[c, :, i * layers : (i + 1) * layers, :].reshape(extent, extent)
            field = jnp.concatenate([space[0, l] * local_pot, space[1, l] * local_pot], axis=1)
            fallen.append(dot(stacked(field, 1), down_b_ref[...]))
        products = dot(down_a_ref[...], stacked(jnp.concatenate(fallen, axis=1), 0))
        for i in range(batch):
            product = products[:, i * 2 * half : (i + 1) * 2 * half]
            swap = pltpu.roll(product[half:], half, 1)
            total = product[:half] + jnp.where(lane_half < half, swap, -swap)
            for part in range(2):
                block = total[:, part * half : (part + 1) * half]
                for h in range(halves):
                    sides = [block[q * FINE : (q + 1) * FINE] for q in range(h * per, (h + 1) * per)]
                    line = jnp.concatenate(sides, axis=1)
                    at = part * layers + c * batch + i
                    mesh[h, pl.ds(at, FINE, stride=rows_msg), :] = line

    wide = 4
    rounds = count // wide
    left = jnp.concatenate(split(jnp.concatenate([mesh[h] for h in range(halves)], axis=1)), axis=0)

    def give(other):
        pltpu.make_async_remote_copy(
            src_ref=back.at[other],
            dst_ref=back_in.at[me],
            send_sem=send_sem.at[3],
            recv_sem=recv_sem.at[3],
            device_id={"ga": other},
        ).start()

    def first_of(i):
        return lax.div(peer((rounds - 1 - i) * wide), wide) * wide

    def find(i):
        span = pl.ds(pl.multiple_of(first_of(i) * LANES, wide * LANES), wide * LANES)
        return dot(left, pick[:, span])

    found = find(0)
    for i in range(rounds):
        following = find(i + 1) if i + 1 < rounds else None
        for k in range(wide):
            here = jnp.broadcast_to(fines[first_of(i) + k], (rows_msg, LANES))
            tile = jnp.zeros((rows_msg, LANES), F32)
            for f in range(FINE):
                cut = (slice(f * rows_msg, (f + 1) * rows_msg), slice(k * LANES, (k + 1) * LANES))
                tile = tile + jnp.where(here == f, found[:rows_mesh][cut] + found[rows_mesh:][cut], 0.0)
            back[first_of(i) + k] = tile
        if i > 0:
            for step in range(wide):
                give(peer((rounds - i) * wide + wide - 1 - step))
        found = following
    for step in range(wide - 1):
        give(peer(wide - 1 - step))
    pltpu.make_async_copy(back.at[me], back_in.at[me], recv_sem.at[3]).start()
    rest.wait()

    def add(t, carry):
        at = pl.ds(pl.multiple_of(t * 16, 16), 16)
        added[at, :] = orb[0, at, :] + orb[1, at, :]
        return carry

    lax.fori_loop(0, bands_all // 16, add, 0)
    load_last.wait()
    arrive(back_in, 3)

    sub_half = lax.broadcasted_iota(jnp.int32, (half, LANES), 0).astype(F32)
    final = dot(last_ref[...], stacked(back_in[...].reshape(count * rows_msg, LANES), 0))
    high, low = split(final)
    final_cat = jnp.concatenate([high, low], axis=1)
    place_rows = jnp.concatenate([place[...], place[...]], axis=0)
    spread_back = dot(final_cat, place_rows)
    for r in range(blocks):
        at_depth = sub_half == colrow[1, r : r + 1, :]
        span = slice(r * LANES, (r + 1) * LANES)
        k_row = kin[r : r + 1, :]
        for part in range(2):
            block = spread_back[part * half : (part + 1) * half, span]
            value = jnp.sum(jnp.where(at_depth, block, 0.0), axis=0, keepdims=True)
            applied_ref[part, r : r + 1, :] = value + k_row * orb[part, 0:1, span]

    u, v = applied_ref[0], applied_ref[1]
    mixed[0], mixed[1], mixed[2] = u, u - v, u + v
    tile_rows = 64
    owners = tile_rows // sub_rows
    spans = count // owners
    low = owners.bit_length() - 1

    def tile_of(t):
        return lax.div(turned(spans - 1 - t, low), owners) if spans > 1 else lax.div(me, owners)

    def sweep(t, slot):
        at = pl.ds(pl.multiple_of(tile_of(t) * tile_rows, tile_rows), tile_rows)
        acc = [jnp.zeros((tile_rows, LANES), F32) for _ in range(3)]
        for r in range(blocks):
            span = slice(r * LANES, (r + 1) * LANES)
            acc[0] = acc[0] + added[at, span] * mixed[0, r : r + 1, :]
            acc[1] = acc[1] + orb[1, at, span] * mixed[1, r : r + 1, :]
            acc[2] = acc[2] + orb[0, at, span] * mixed[2, r : r + 1, :]
        sums[slot, 0] = acc[0] - acc[1]
        sums[slot, 1] = acc[2] - acc[0]

    def narrow(t, slot):
        both = sums[slot].reshape(2 * tile_rows, LANES)
        line = jnp.sum(jnp.transpose(both), axis=0, keepdims=True)
        sub_out[t] = line * (1.0 / (slots * count))

    def share(t):
        base = turned(spans - 1 - t, low) if spans > 1 else me
        near = [peer(step) - me for step in range(owners - 1, -1, -1)]
        return [base + step for step in near]

    def publish(t, other):
        pltpu.make_async_remote_copy(
            src_ref=sub_out.at[t],
            dst_ref=sub_in.at[me],
            send_sem=send_sem.at[4],
            recv_sem=recv_sem.at[4],
            device_id={"ga": other},
        ).start()

    def sub_step(t, carry):
        narrow(t - 1, lax.rem(t - 1, 2))
        sweep(t, lax.rem(t, 2))
        for other in share(t - 1):
            publish(t - 1, other)
        return carry

    sweep(0, 0)
    lax.fori_loop(1, spans, sub_step, 0)
    narrow(spans - 1, (spans - 1) % 2)
    for other in share(spans - 1)[:-1]:
        publish(spans - 1, other)
    pltpu.make_async_copy(sub_out.at[spans - 1], sub_in.at[me], recv_sem.at[4]).start()
    arrive(sub_in, 4)
    total = jnp.broadcast_to(jnp.sum(sub_in[...], axis=0), (8, LANES))
    offset = lax.rem(me, owners) * sub_rows
    mine = pltpu.roll(total, lax.rem(LANES - offset, LANES), 1)
    sub_ref[0] = mine[0:1, :sub_rows]
    sub_ref[1] = mine[0:1, tile_rows : tile_rows + sub_rows]
    if not narrow_msg:
        sent(ids_out, 0)
    sent(msg, 1)
    for c in range(layers // batch):
        sent(pot_out.at[c], 2)
    sent(back, 3)
    sub_view = sub_in.at[pl.ds(0, count - 1)]
    pltpu.make_async_copy(sub_view, sub_view, send_sem.at[4]).wait()


def emit(applied_ref, sub_ref, applied_out, sub_out):
    applied_out[...] = applied_ref[...]
    sub_out[...] = sub_ref[...]


def local(orbitals, coeff_cells, potential):
    count = lax.axis_size("ga")
    extent = potential.shape[1]
    layers = extent // count
    half = extent // 2
    bands_all, slots = orbitals.shape[1], orbitals.shape[2]
    blocks = slots // LANES
    parts = 2 * layers
    rows_msg = -(-parts // 8) * 8
    sub_rows = bands_all // count
    group = 8
    narrow = int(is_narrow(extent, count, parts))
    batch = min(2, layers)
    folds = half // FINE
    constants = [jnp.asarray(t) for t in tables(extent, count, rows_msg)]
    vmem = pl.BlockSpec(memory_space=pltpu.VMEM)
    staged = [(blocks, LANES), (layers, extent, extent)] + [t.shape for t in constants]
    kinds = [jnp.int32, F32] + [BF] * len(constants)
    scratch = [pltpu.VMEM(shape, kind) for shape, kind in zip(staged, kinds)] + [
        pltpu.VMEM((2, bands_all, slots), F32),
        pltpu.VMEM((LANES, slots), BF),
        pltpu.VMEM((count, 1, LANES), F32),
        pltpu.VMEM((count, 1, LANES), F32),
        pltpu.VMEM((count, rows_msg - narrow, LANES), F32),
        pltpu.VMEM((count, rows_msg - narrow, LANES), F32),
        pltpu.VMEM((layers // batch, count, batch * layers, LANES), F32),
        pltpu.VMEM((layers // batch, count, batch * layers, LANES), F32),
        pltpu.VMEM((folds * half, count * LANES), BF),
        pltpu.VMEM((count, 1, LANES), F32),
        pltpu.VMEM((2 * FINE * rows_msg, folds * half), F32),
        pltpu.VMEM((folds * half // LANES, FINE * rows_msg, LANES), F32),
        pltpu.VMEM((count, rows_msg, LANES), F32),
        pltpu.VMEM((count, rows_msg, LANES), F32),
        pltpu.VMEM((2, 2, 64, LANES), F32),
        pltpu.VMEM((bands_all // 64, 1, LANES), F32),
        pltpu.VMEM((count, 1, LANES), F32),
        pltpu.VMEM((bands_all, slots), F32),
        pltpu.VMEM((3, blocks, LANES), F32),
        pltpu.VMEM((blocks, LANES), F32),
        pltpu.VMEM((4, blocks, LANES), F32),
        pltpu.VMEM((2, layers, extent, extent), F32),
        pltpu.SemaphoreType.DMA,
        pltpu.SemaphoreType.DMA,
        pltpu.SemaphoreType.DMA((len(staged),)),
        pltpu.SemaphoreType.DMA((5,)),
        pltpu.SemaphoreType.DMA((5,)),
        pltpu.SemaphoreType.DMA((count // group,)),
        pltpu.SemaphoreType.DMA((count // group,)),
        pltpu.SemaphoreType.DMA((layers // batch,)),
    ]
    applied, sub = pl.pallas_call(
        functools.partial(kernel, count, layers, extent, rows_msg, group),
        out_shape=(
            pltpu.VMEM((2, blocks, LANES), F32),
            pltpu.VMEM((2, 1, sub_rows), F32),
        ),
        in_specs=[pl.BlockSpec(memory_space=pl.ANY)] * (3 + len(constants)),
        out_specs=(vmem, vmem),
        scratch_shapes=scratch,
        compiler_params=pltpu.CompilerParams(
            collective_id=0, has_side_effects=True, vmem_limit_bytes=60 * 1024 * 1024
        ),
    )(coeff_cells.reshape(blocks, LANES), potential, *constants, orbitals)
    applied, sub = pl.pallas_call(
        emit,
        out_shape=(
            jax.ShapeDtypeStruct(applied.shape, F32),
            jax.ShapeDtypeStruct(sub.shape, F32),
        ),
        in_specs=[vmem, vmem],
        out_specs=(vmem, vmem),
        compiler_params=pltpu.CompilerParams(vmem_limit_bytes=1024 * 1024),
    )(applied, sub)
    applied = applied.reshape(2, 1, slots)
    subspace = jnp.transpose(sub, (2, 0, 1))
    return applied, subspace


def solution(mesh):
    in_specs = (P(None, "kpt", "ga"), P("ga"), P("ga", None, None))
    out_specs = (P(None, "kpt", "ga"), P("ga", None, "kpt"))
    return jax.shard_map(local, mesh=mesh, in_specs=in_specs, out_specs=out_specs, check_vma=False)
```

```python
import functools

import jax
import jax.numpy as jnp
import ml_dtypes
import numpy as np
from jax import lax
from jax.experimental import pallas as pl
from jax.experimental.pallas import tpu as pltpu
from jax.sharding import PartitionSpec as P

RADIUS = 30
BF = jnp.bfloat16
F32 = jnp.float32
LANES = 128
FINE = 16
NN = (((1,), (0,)), ((), ()))
NT = (((1,), (1,)), ((), ()))


def split_np(table):
    high = table.astype(np.float32).astype(ml_dtypes.bfloat16)
    low = (table - high.astype(np.float64)).astype(np.float32).astype(ml_dtypes.bfloat16)
    return high, low


def stack_np(table, axis):
    high, low = split_np(table)
    return np.concatenate([high, high, low], axis=axis)


def phases(extent, half):
    index = np.arange(half)
    freq = np.where(index < half // 2, index, index - half)
    angle = 2.0 * np.pi * ((np.arange(extent)[:, None] * freq[None, :]) % extent) / extent
    return np.cos(angle), np.sin(angle)


@functools.lru_cache(None)
def tables(extent, count, rows_msg, batch):
    half = extent // 2
    layers = extent // count
    cos, sin = phases(extent, half)
    first = np.zeros((count, rows_msg, 2 * half))
    last = np.zeros((2 * half, count, rows_msg))
    for l in range(layers):
        z = np.arange(count) * layers + l
        first[:, l, :half], first[:, l, half:] = cos[z], -sin[z]
        first[:, layers + l, :half], first[:, layers + l, half:] = sin[z], cos[z]
        last[:half, :, l], last[:half, :, layers + l] = cos[z].T, sin[z].T
        last[half:, :, l], last[half:, :, layers + l] = -sin[z].T, cos[z].T
    first = first.reshape(count * rows_msg, 2 * half)
    order = [
        part * layers + c * batch + i
        for c in range(layers // batch)
        for part in range(2)
        for i in range(batch)
    ]
    last = last[:, :, order].reshape(2 * half, count, layers // batch, 2 * batch)
    last = last.transpose(0, 2, 1, 3).reshape(2 * half, 2 * layers * count) / float(extent) ** 3
    up_a = np.block([[cos, -sin], [sin, cos]])
    up_b = np.concatenate([cos.T, sin.T], axis=1)
    down_b = np.block([[cos, -sin], [sin, cos]])
    down_a = np.concatenate([cos.T, sin.T], axis=0)
    up_b_high, up_b_low = split_np(up_b)
    return (
        stack_np(first, 1),
        stack_np(up_a, 1),
        np.concatenate([up_b_high, up_b_high, up_b_low, np.zeros_like(up_b_low)]),
        stack_np(down_b, 0),
        stack_np(down_a, 1),
        stack_np(last, 1),
    )


def sheared(values, shifts):
    row = lax.broadcasted_iota(jnp.int32, values.shape, 0) % 4
    turned = [pltpu.roll(values, shift, 1) for shift in shifts]
    return jnp.where(row == 0, turned[0], jnp.where(row == 1, turned[1], turned[2]))


def most_columns(extent, count):
    index = np.arange(extent)
    square = np.where(index < extent // 2, index, index - extent) ** 2
    return -(-int((square[:, None] + square[None, :] <= RADIUS * RADIUS).sum()) // count)


def is_narrow(extent, count, parts):
    return parts == 8 and most_columns(extent, count) <= 3 * (LANES // 4)


def dot(left, right, dims=NN):
    return lax.dot_general(left, right, dims, preferred_element_type=F32)


def split(values):
    high = values.astype(BF)
    return high, (values - high.astype(F32)).astype(BF)


def stacked(values, axis):
    high, low = split(values)
    return jnp.concatenate([high, low, high], axis=axis)


def signed(values, extent):
    return jnp.where(values < extent // 2, values, values - extent)


def rows_iota(rows):
    return lax.broadcasted_iota(jnp.int32, (rows, LANES), 0).astype(F32).astype(BF)


def tall(row, rows):
    block = jnp.broadcast_to(row, (16, LANES)).astype(BF)
    return jnp.concatenate([block] * (rows // 16), axis=0)


def matches(index, row):
    return jnp.where(index == tall(row, index.shape[0]), BF(1.0), BF(0.0))


def bits_of(number, width):
    return [lax.rem(lax.div(number, 2**k), 2) for k in range(width)]


def kernel(
    count, layers, extent, rows_msg, group,
    cells_hbm, pot_hbm, first_hbm, up_a_hbm, up_b_hbm, down_b_hbm, down_a_hbm, last_hbm,
    orb_hbm, applied_ref, sub_ref,
    cells_ref, pot_ref, first_ref, up_a_ref, up_b_ref, down_b_ref, down_a_ref, last_ref,
    orb, place, ids_out, ids_in, msg, arrived, pot_out, pot_in,
    pick, fines, grid, mesh, freq, back, back_in, sums, sub_out, sub_in, added, mixed, kin, colrow, space,
    win_sem, orb_sem, load_sem, send_sem, recv_sem, ids_sem, msg_sem, pot_sem, back_sem,
):
    me = lax.axis_index("ga")
    half = extent // 2
    slots = orb.shape[2]
    blocks = slots // LANES
    bands_all = orb.shape[1]
    sub_rows = bands_all // count
    parts = 2 * layers
    batch = min(2, layers)
    folds = half // FINE
    narrow_msg = is_narrow(extent, count, parts)
    room = 3 * (LANES // 4)
    width = count.bit_length() - 1
    turns = [(1 - 2 * bit) * 2**k for k, bit in enumerate(bits_of(me, width))]

    def peer(step):
        return me + sum([turns[k] for k in range(width) if step >> k & 1], 0)

    def turned(step, low):
        wide = width - low
        return me + sum([bit * turns[low + k] for k, bit in enumerate(bits_of(step, wide))], 0)

    far_first = [peer(step) for step in range(count - 1, 0, -1)]
    barrier = pltpu.get_barrier_semaphore()
    load_cells = pltpu.make_async_copy(cells_hbm, cells_ref, load_sem.at[0])
    load_cells.start()
    head = pltpu.make_async_copy(orb_hbm.at[:, 0:8, :], orb.at[:, 0:8, :], win_sem)
    head.start()
    for other in far_first:
        pl.semaphore_signal(barrier, inc=1, device_id={"ga": other})
    sources = (first_hbm, pot_hbm, up_a_hbm, up_b_hbm, down_b_hbm, down_a_hbm, last_hbm)
    targets = (first_ref, pot_ref, up_a_ref, up_b_ref, down_b_ref, down_a_ref, last_ref)
    loads = [
        pltpu.make_async_copy(source, target, load_sem.at[i + 1])
        for i, (source, target) in enumerate(zip(sources, targets))
    ]
    load_first, load_pot, load_up_a, load_up_b, load_down_b, load_down_a, load_last = loads
    for load in loads:
        load.start()
    rest = pltpu.make_async_copy(orb_hbm.at[:, 8:, :], orb.at[:, 8:, :], orb_sem)
    rest.start()
    groups = count // group
    my_group = me // group

    def exchange(source, target, phase, landed):
        own = pltpu.make_async_copy(source.at[me], target.at[me], landed)
        own.start()

        for other in far_first:
            pltpu.make_async_remote_copy(
                src_ref=source.at[other],
                dst_ref=target.at[me],
                send_sem=send_sem.at[phase],
                recv_sem=landed,
                device_id={"ga": other},
            ).start()

    def arrive(target, phase):
        pltpu.make_async_copy(target, target, recv_sem.at[phase]).wait()

    def sent(source, phase):
        view = source.at[pl.ds(0, count - 1)]
        pltpu.make_async_copy(view, view, send_sem.at[phase]).wait()

    load_cells.wait()
    cells = cells_ref[...]
    live = cells >= 0
    column = jnp.right_shift(cells, extent.bit_length() - 1)
    rolled = pltpu.roll(column, 1, 1)
    lane = lax.broadcasted_iota(jnp.int32, cells.shape, 1)
    row = lax.broadcasted_iota(jnp.int32, cells.shape, 0)
    earlier = jnp.where(lane == 0, pltpu.roll(rolled, 1, 0), rolled)
    earlier = jnp.where((lane == 0) & (row == 0), -1, earlier)
    starts = live & (column != earlier)
    flags = starts.astype(F32).astype(BF)
    sq = lambda axis: lax.broadcasted_iota(jnp.int32, (LANES, LANES), axis)
    upper = (sq(0) <= sq(1)).astype(F32).astype(BF)
    inner = dot(flags, upper)
    totals = dot(flags, jnp.ones((LANES, LANES), BF))
    below = lax.broadcasted_iota(jnp.int32, (blocks, blocks), 1) < lax.broadcasted_iota(
        jnp.int32, (blocks, blocks), 0
    )
    outer = dot(below.astype(F32).astype(BF), totals.astype(BF))
    local = (inner + outer - 1.0).astype(jnp.int32)
    local = jnp.where(live, local, -1)
    safe = jnp.where(live, cells, 0)
    plane_c = safe % extent
    plane_b = safe // extent % extent
    plane_a = safe // (extent * extent)
    fa, fb, fc = signed(plane_a, extent), signed(plane_b, extent), signed(plane_c, extent)
    kinetic = (fa * fa + fb * fb + fc * fc).astype(F32) / (RADIUS * RADIUS)
    kin[...] = jnp.where(live, kinetic, 0.0)
    small_a = plane_a % half
    colrow[0] = local.astype(F32)
    colrow[1] = (plane_c % half).astype(F32)
    colrow[2] = jnp.where(starts, small_a % FINE, 0).astype(F32)
    colrow[3] = jnp.where(starts, small_a // FINE * half + plane_b % half, 0).astype(F32)

    head.wait()
    deep = rows_iota(half)
    full = rows_iota(LANES)
    sub_ids = lax.broadcasted_iota(jnp.int32, (16, LANES), 0)
    chunk = 4
    sticks = jnp.zeros((4 * half + 16, LANES), F32)
    for c in range(blocks // chunk):
        pieces = []
        for r in range(c * chunk, (c + 1) * chunk):
            span = slice(r * LANES, (r + 1) * LANES)
            at_depth = matches(deep, colrow[1, r : r + 1, :])
            lines = []
            for part in range(2):
                for value in split(orb[part, 0:1, span]):
                    lines.append(at_depth * tall(value.astype(F32), half))
            is_fine, is_wide = colrow[2, r : r + 1, :], colrow[3, r : r + 1, :]
            tail = jnp.where(sub_ids == 0, is_fine, jnp.where(sub_ids == 1, is_wide, 0.0))
            pieces.append(jnp.concatenate(lines + [tail.astype(BF)], axis=0))
            place[:, span] = matches(full, colrow[0, r : r + 1, :])
        span = slice(c * chunk * LANES, (c + 1) * chunk * LANES)
        sticks = sticks + dot(jnp.concatenate(pieces, axis=1), place[:, span], NT)
    code = sticks[4 * half : 4 * half + 1] * (folds * half) + sticks[4 * half + 1 : 4 * half + 2]

    both = jnp.concatenate(
        [
            sticks[0:half] + sticks[half : 2 * half],
            sticks[2 * half : 3 * half] + sticks[3 * half : 4 * half],
        ],
        axis=0,
    )
    load_first.wait()
    sheet = dot(first_ref[...], stacked(both, 0)).reshape(count, rows_msg, LANES)
    if narrow_msg:
        row_of = lax.broadcasted_iota(jnp.int32, (count, rows_msg, LANES), 1)
        lane_of = lax.broadcasted_iota(jnp.int32, (count, rows_msg, LANES), 2)
        ends = jnp.where(row_of < 4, sheet[:, rows_msg - 1 : rows_msg, :], code[None])
        ends = ends.reshape(count * rows_msg, LANES)
        ends = sheared(ends, [room, room - LANES // 4, room - LANES // 2])
        sheet = jnp.where(lane_of < room, sheet, ends.reshape(count, rows_msg, LANES))
        msg[...] = sheet[:, : rows_msg - 1, :]
    else:
        msg[...] = sheet
        ids_out[...] = jnp.broadcast_to(code[None], ids_out.shape)
    load_pot.wait()
    for a in range(layers):
        across = jnp.transpose(pot_ref[a])
        for d in range(count):
            for l in range(layers):
                row = l % batch * layers + a
                pot_out[l // batch, d, row : row + 1, :] = across[d * layers + l : d * layers + l + 1]
    pl.semaphore_wait(barrier, count - 1)
    if not narrow_msg:
        exchange(ids_out, ids_in, 0, ids_sem.at[my_group])
    exchange(msg, arrived, 1, msg_sem.at[my_group])

    for c in range(layers // batch):
        exchange(pot_out.at[c], pot_in.at[c], 2, pot_sem.at[c])

    grid[...] = jnp.zeros_like(grid)
    broad = rows_iota(folds * half)
    row_of = lax.broadcasted_iota(jnp.int32, (rows_msg, LANES), 0)
    lane_of = lax.broadcasted_iota(jnp.int32, (rows_msg, LANES), 1)

    def gather_group(step, carry):
        g = lax.div(turned(step, group.bit_length() - 1), group)
        if not narrow_msg:
            ids_view = ids_in.at[pl.ds(g * group, group)]
            pltpu.make_async_copy(ids_view, ids_view, ids_sem.at[g]).wait()
        msg_view = arrived.at[pl.ds(g * group, group)]
        pltpu.make_async_copy(msg_view, msg_view, msg_sem.at[g]).wait()
        pieces = []
        for k in range(group):
            d = g * group + k
            tile = arrived[d]
            if narrow_msg:
                tile = jnp.concatenate([tile, tile[0:1]], axis=0)
                ends = sheared(tile, [LANES // 4, LANES // 2, room])
                ends = jnp.where(lane_of // (LANES // 4) == row_of % 4, ends, 0.0)
                ends = jnp.where(row_of % 4 < 3, ends, 0.0)
                final_row = ends[0:1] + ends[1:2] + ends[2:3]
                code = ends[4:5] + ends[5:6] + ends[6:7]
                tile = jnp.where(row_of == rows_msg - 1, final_row, tile)
                tile = jnp.where(lane_of < room, tile, 0.0)
            else:
                code = ids_in[d]
            is_fine = jnp.floor(code * (1.0 / (folds * half)))
            fines[d] = is_fine
            span = pl.ds(pl.multiple_of(d * LANES, LANES), LANES)
            pick[:, span] = matches(broad, code - is_fine * (folds * half))
            high, low = split(tile)
            high, low = high.astype(F32), low.astype(F32)
            here = jnp.broadcast_to(is_fine, (rows_msg, LANES))
            lines = [jnp.where(here == f, high, 0.0) for f in range(FINE)]
            lines += [jnp.where(here == f, low, 0.0) for f in range(FINE)]
            pieces.append(jnp.concatenate(lines, axis=0).astype(BF))
        span = pl.ds(pl.multiple_of(g * group * LANES, group * LANES), group * LANES)
        grid[...] += dot(jnp.concatenate(pieces, axis=1), pick[:, span], NT)
        return carry

    lax.fori_loop(0, groups, gather_group, 0)
    load_up_a.wait()
    load_up_b.wait()
    load_down_b.wait()
    load_down_a.wait()

    rows_mesh = FINE * rows_msg
    halves = folds * half // LANES
    per = LANES // half
    both = grid[0:rows_mesh] + grid[rows_mesh:]
    for h in range(halves):
        mesh[h] = both[:, h * LANES : (h + 1) * LANES]

    lines = []
    for part in range(2):
        for h in range(halves):
            blocks_of = [
                mesh[h, pl.ds(part * layers + l, FINE, stride=rows_msg), :] for l in range(layers)
            ]
            for q in range(per):
                lines.append(
                    jnp.concatenate([block[:, q * half : (q + 1) * half] for block in blocks_of], axis=1)
                )
    lifted = dot(up_a_ref[...], stacked(jnp.concatenate(lines, axis=0), 0))
    for l in range(layers):
        plane = lifted[:, l * half : (l + 1) * half]
        high = plane.astype(BF).astype(F32)
        pair = jnp.concatenate([high, plane - high], axis=1).astype(BF)
        whole = dot(jnp.concatenate([pair, pair], axis=1), up_b_ref[...])
        space[0, l] = whole[:extent, :extent] - whole[extent:, extent:]
        space[1, l] = whole[:extent, extent:] + whole[extent:, :extent]

    rows_back = 2 * batch
    share_of = 8 // rows_back
    wide = 8
    rounds = count // wide
    sub_of = (lax.broadcasted_iota(jnp.int32, (8, LANES), 0) // rows_back).astype(F32)

    def first_of(i):
        return lax.div(peer((rounds - 1 - i) * wide), wide) * wide

    def give(c, other):
        pltpu.make_async_remote_copy(
            src_ref=back.at[c, other],
            dst_ref=back_in.at[c, me],
            send_sem=send_sem.at[3],
            recv_sem=back_sem.at[c],
            device_id={"ga": other},
        ).start()

    def take(c):
        sheet = jnp.concatenate([freq[c, h] for h in range(halves)], axis=1)
        left = jnp.concatenate(split(sheet), axis=0)
        rows_freq = FINE * rows_back

        def find(i):
            span = pl.ds(pl.multiple_of(first_of(i) * LANES, wide * LANES), wide * LANES)
            return dot(left, pick[:, span])

        found = find(0)
        for i in range(rounds):
            following = find(i + 1) if i + 1 < rounds else None
            for k in range(wide):
                here = jnp.broadcast_to(fines[first_of(i) + k], (8, LANES)) - sub_of
                tile = jnp.zeros((8, LANES), F32)
                for m in range(FINE // share_of):
                    at = (slice(m * 8, (m + 1) * 8), slice(k * LANES, (k + 1) * LANES))
                    block = found[:rows_freq][at] + found[rows_freq:][at]
                    tile = tile + jnp.where(here == m * share_of, block, 0.0)
                shift = 4
                while shift >= rows_back:
                    tile = tile + pltpu.roll(tile, shift, 0)
                    shift //= 2
                back[c, first_of(i) + k] = tile[0:rows_back]
            if i > 0:
                for step in range(wide):
                    give(c, peer((rounds - i) * wide + wide - 1 - step))
            found = following
        for step in range(wide - 1):
            give(c, peer(wide - 1 - step))
        pltpu.make_async_copy(back.at[c, me], back_in.at[c, me], back_sem.at[c]).start()

    lane_half = lax.broadcasted_iota(jnp.int32, (half, 2 * half), 1)
    for c in range(layers // batch):
        pltpu.make_async_copy(pot_in.at[c], pot_in.at[c], pot_sem.at[c]).wait()
        fallen = []
        for i in range(batch):
            l = c * batch + i
            local_pot = pot_in[c, :, i * layers : (i + 1) * layers, :].reshape(extent, extent)
            field = jnp.concatenate([space[0, l] * local_pot, space[1, l] * local_pot], axis=1)
            fallen.append(dot(stacked(field, 1), down_b_ref[...]))
        products = dot(down_a_ref[...], stacked(jnp.concatenate(fallen, axis=1), 0))
        for i in range(batch):
            product = products[:, i * 2 * half : (i + 1) * 2 * half]
            swap = pltpu.roll(product[half:], half, 1)
            total = product[:half] + jnp.where(lane_half < half, swap, -swap)
            for part in range(2):
                block = total[:, part * half : (part + 1) * half]
                for h in range(halves):
                    sides = [block[q * FINE : (q + 1) * FINE] for q in range(h * per, (h + 1) * per)]
                    line = jnp.concatenate(sides, axis=1)
                    freq[c, h, pl.ds(part * batch + i, FINE, stride=rows_back), :] = line
        take(c)

    rest.wait()

    def add(t, carry):
        at = pl.ds(pl.multiple_of(t * 16, 16), 16)
        added[at, :] = orb[0, at, :] + orb[1, at, :]
        return carry

    lax.fori_loop(0, bands_all // 16, add, 0)
    load_last.wait()
    for c in range(layers // batch):
        pltpu.make_async_copy(back_in.at[c], back_in.at[c], back_sem.at[c]).wait()

    sub_half = lax.broadcasted_iota(jnp.int32, (half, LANES), 0).astype(F32)
    final = dot(last_ref[...], stacked(back_in[...].reshape(parts * count, LANES), 0))
    high, low = split(final)
    final_cat = jnp.concatenate([high, low], axis=1)
    place_rows = jnp.concatenate([place[...], place[...]], axis=0)
    spread_back = dot(final_cat, place_rows)
    for r in range(blocks):
        at_depth = sub_half == colrow[1, r : r + 1, :]
        span = slice(r * LANES, (r + 1) * LANES)
        k_row = kin[r : r + 1, :]
        for part in range(2):
            block = spread_back[part * half : (part + 1) * half, span]
            value = jnp.sum(jnp.where(at_depth, block, 0.0), axis=0, keepdims=True)
            applied_ref[part, r : r + 1, :] = value + k_row * orb[part, 0:1, span]

    u, v = applied_ref[0], applied_ref[1]
    mixed[0], mixed[1], mixed[2] = u, u - v, u + v
    tile_rows = 64
    owners = tile_rows // sub_rows
    spans = count // owners
    low = owners.bit_length() - 1

    def tile_of(t):
        return lax.div(turned(spans - 1 - t, low), owners) if spans > 1 else lax.div(me, owners)

    def sweep(t, slot):
        at = pl.ds(pl.multiple_of(tile_of(t) * tile_rows, tile_rows), tile_rows)
        acc = [jnp.zeros((tile_rows, LANES), F32) for _ in range(3)]
        for r in range(blocks):
            span = slice(r * LANES, (r + 1) * LANES)
            acc[0] = acc[0] + added[at, span] * mixed[0, r : r + 1, :]
            acc[1] = acc[1] + orb[1, at, span] * mixed[1, r : r + 1, :]
            acc[2] = acc[2] + orb[0, at, span] * mixed[2, r : r + 1, :]
        sums[slot, 0] = acc[0] - acc[1]
        sums[slot, 1] = acc[2] - acc[0]

    def narrow(t, slot):
        both = sums[slot].reshape(2 * tile_rows, LANES)
        line = jnp.sum(jnp.transpose(both), axis=0, keepdims=True)
        sub_out[t] = line * (1.0 / (slots * count))

    def share(t):
        base = turned(spans - 1 - t, low) if spans > 1 else me
        near = [peer(step) - me for step in range(owners - 1, -1, -1)]
        return [base + step for step in near]

    def publish(t, other):
        pltpu.make_async_remote_copy(
            src_ref=sub_out.at[t],
            dst_ref=sub_in.at[me],
            send_sem=send_sem.at[4],
            recv_sem=recv_sem.at[4],
            device_id={"ga": other},
        ).start()

    def sub_step(t, carry):
        narrow(t - 1, lax.rem(t - 1, 2))
        sweep(t, lax.rem(t, 2))
        for other in share(t - 1):
            publish(t - 1, other)
        return carry

    sweep(0, 0)
    lax.fori_loop(1, spans - 1, sub_step, 0)
    narrow(spans - 2, (spans - 2) % 2)
    for other in share(spans - 2):
        publish(spans - 2, other)
    sweep(spans - 1, (spans - 1) % 2)
    narrow(spans - 1, (spans - 1) % 2)
    for other in share(spans - 1)[:-1]:
        publish(spans - 1, other)
    pltpu.make_async_copy(sub_out.at[spans - 1], sub_in.at[me], recv_sem.at[4]).start()
    arrive(sub_in, 4)
    total = jnp.broadcast_to(jnp.sum(sub_in[...], axis=0), (8, LANES))
    offset = lax.rem(me, owners) * sub_rows
    mine = pltpu.roll(total, lax.rem(LANES - offset, LANES), 1)
    sub_ref[0] = mine[0:1, :sub_rows]
    sub_ref[1] = mine[0:1, tile_rows : tile_rows + sub_rows]
    if not narrow_msg:
        sent(ids_out, 0)
    sent(msg, 1)
    for c in range(layers // batch):
        sent(pot_out.at[c], 2)
    for c in range(layers // batch):
        sent(back.at[c], 3)
    sub_view = sub_in.at[pl.ds(0, count - 1)]
    pltpu.make_async_copy(sub_view, sub_view, send_sem.at[4]).wait()


def emit(applied_ref, sub_ref, applied_out, sub_out):
    applied_out[...] = applied_ref[...]
    sub_out[...] = sub_ref[...]


def local(orbitals, coeff_cells, potential):
    count = lax.axis_size("ga")
    extent = potential.shape[1]
    layers = extent // count
    half = extent // 2
    bands_all, slots = orbitals.shape[1], orbitals.shape[2]
    blocks = slots // LANES
    parts = 2 * layers
    rows_msg = -(-parts // 8) * 8
    sub_rows = bands_all // count
    group = 8
    narrow = int(is_narrow(extent, count, parts))
    batch = min(2, layers)
    folds = half // FINE
    constants = [jnp.asarray(t) for t in tables(extent, count, rows_msg, batch)]
    vmem = pl.BlockSpec(memory_space=pltpu.VMEM)
    staged = [(blocks, LANES), (layers, extent, extent)] + [t.shape for t in constants]
    kinds = [jnp.int32, F32] + [BF] * len(constants)
    scratch = [pltpu.VMEM(shape, kind) for shape, kind in zip(staged, kinds)] + [
        pltpu.VMEM((2, bands_all, slots), F32),
        pltpu.VMEM((LANES, slots), BF),
        pltpu.VMEM((count, 1, LANES), F32),
        pltpu.VMEM((count, 1, LANES), F32),
        pltpu.VMEM((count, rows_msg - narrow, LANES), F32),
        pltpu.VMEM((count, rows_msg - narrow, LANES), F32),
        pltpu.VMEM((layers // batch, count, batch * layers, LANES), F32),
        pltpu.VMEM((layers // batch, count, batch * layers, LANES), F32),
        pltpu.VMEM((folds * half, count * LANES), BF),
        pltpu.VMEM((count, 1, LANES), F32),
        pltpu.VMEM((2 * FINE * rows_msg, folds * half), F32),
        pltpu.VMEM((folds * half // LANES, FINE * rows_msg, LANES), F32),
        pltpu.VMEM((layers // batch, folds * half // LANES, FINE * 2 * batch, LANES), F32),
        pltpu.VMEM((layers // batch, count, 2 * batch, LANES), F32),
        pltpu.VMEM((layers // batch, count, 2 * batch, LANES), F32),
        pltpu.VMEM((2, 2, 64, LANES), F32),
        pltpu.VMEM((bands_all // 64, 1, LANES), F32),
        pltpu.VMEM((count, 1, LANES), F32),
        pltpu.VMEM((bands_all, slots), F32),
        pltpu.VMEM((3, blocks, LANES), F32),
        pltpu.VMEM((blocks, LANES), F32),
        pltpu.VMEM((4, blocks, LANES), F32),
        pltpu.VMEM((2, layers, extent, extent), F32),
        pltpu.SemaphoreType.DMA,
        pltpu.SemaphoreType.DMA,
        pltpu.SemaphoreType.DMA((len(staged),)),
        pltpu.SemaphoreType.DMA((5,)),
        pltpu.SemaphoreType.DMA((5,)),
        pltpu.SemaphoreType.DMA((count // group,)),
        pltpu.SemaphoreType.DMA((count // group,)),
        pltpu.SemaphoreType.DMA((layers // batch,)),
        pltpu.SemaphoreType.DMA((layers // batch,)),
    ]
    applied, sub = pl.pallas_call(
        functools.partial(kernel, count, layers, extent, rows_msg, group),
        out_shape=(
            pltpu.VMEM((2, blocks, LANES), F32),
            pltpu.VMEM((2, 1, sub_rows), F32),
        ),
        in_specs=[pl.BlockSpec(memory_space=pl.ANY)] * (3 + len(constants)),
        out_specs=(vmem, vmem),
        scratch_shapes=scratch,
        compiler_params=pltpu.CompilerParams(
            collective_id=0, has_side_effects=True, vmem_limit_bytes=60 * 1024 * 1024
        ),
    )(coeff_cells.reshape(blocks, LANES), potential, *constants, orbitals)
    applied, sub = pl.pallas_call(
        emit,
        out_shape=(
            jax.ShapeDtypeStruct(applied.shape, F32),
            jax.ShapeDtypeStruct(sub.shape, F32),
        ),
        in_specs=[vmem, vmem],
        out_specs=(vmem, vmem),
        compiler_params=pltpu.CompilerParams(vmem_limit_bytes=1024 * 1024),
    )(applied, sub)
    applied = applied.reshape(2, 1, slots)
    subspace = jnp.transpose(sub, (2, 0, 1))
    return applied, subspace


def solution(mesh):
    in_specs = (P(None, "kpt", "ga"), P("ga"), P("ga", None, None))
    out_specs = (P(None, "kpt", "ga"), P("ga", None, "kpt"))
    return jax.shard_map(local, mesh=mesh, in_specs=in_specs, out_specs=out_specs, check_vma=False)
```
